256 devices in a mesh: groups: 4 (over y, x), blk: 32 (over z), sub: 2 (over core).
Axes of the slice: x: 2, y: 2, z: 32, core: 2. Of those that a mesh axis runs over, the one named last changes fastest.
The devices are a block of a 4x8x32 slice.
Arguments:
- embeddings: bfloat16 [49152, 1024], P(('groups', 'blk', 'sub')), parts along dimension 0, may hold values from -6 to 6
- member_key: int32 [49152], P(('groups', 'blk', 'sub')), parts along dimension 0, may hold values from 0 to 1073741823, as said below
- limit_index: int32 [4], P('groups'), parts along dimension 0, may hold values from 0 to 7
Outputs:
- max_cosine: float32 [49152], P(('groups', 'blk', 'sub')), parts along dimension 0
- kept_share: float32 [4], P('groups'), parts along dimension 0
The draws below stay inside these ranges and needn't reach their ends.
There are 4 independent parts, one for each index of `groups`. The reference program is written for one: setup_inputs(seed, part) draws one part's arguments, and reference() takes and returns one part's arrays. A program takes and returns all parts, laid end to end along the dimension named above; each array names one. Nothing has to cross between parts.
Inputs may be any that keep to these rules, and one draw needn't show every extreme that they name: `member_key`: all keys of a cluster are distinct. A key's quotient by 268435456 is the member's sub-cluster, 0 to 3; its remainder orders the members.
All inputs are finite; a program needn't handle non-finite values.
Results may differ from the reference program's by a relative error of at most 0.0013.
Values may be sent and summed in bfloat16 or wider, within the bound.
No kernel may reach another device: no remote copies, remote signals or barrier semaphores. Data moves between devices by JAX's collectives and lax.ppermute only.
A program may use at most 64 MiB of HBM per device.

```python
import math
import jax
import jax.numpy as jnp
from jax import lax

D = 1024
LABELS = 4
LIMITS = 8
MEMBERS = 12288


label_stride = 268435456


def draw_member_key(key, part):
    spacing = label_stride // MEMBERS
    places = jax.random.permutation(jax.random.fold_in(key, 11), MEMBERS).astype(jnp.int32)
    jitter = jax.random.randint(jax.random.fold_in(key, 12), (MEMBERS,), 0, spacing, dtype=jnp.int32)
    labels = jax.random.randint(jax.random.fold_in(key, 13), (MEMBERS,), 0, LABELS, dtype=jnp.int32)
    return labels * label_stride + places * spacing + jitter


def levels(rng, shape, pieces, low, top_value):
    gain, own = 1.0, jax.random.fold_in(rng, 6)
    for position, parts in pieces:
        heights = jnp.exp(jax.random.uniform(jax.random.fold_in(own, position), (parts,), jnp.float32, low / len(pieces), top_value / len(pieces)))
        gain = gain * jnp.repeat(heights, shape[position] // parts).reshape([-1 if axis == position else 1 for axis in range(len(shape))])
    return gain


def noise(rng, extent, spread, bound, split=(), kind=jnp.bfloat16):
    factor_of = levels(rng, extent, split, -0.22, 0.18) if split else 1.0
    entries = jax.random.normal(rng, extent, jnp.float32) * spread * factor_of
    return jnp.minimum(jnp.maximum(entries, -bound), bound).astype(kind)


def setup_inputs(seed: int = 0, part: int = 0) -> dict:
    key_of = jax.random.split(jax.random.key(seed), 4)
    own_keys = jax.random.split(jax.random.fold_in(key_of[3], part), 4)
    embeddings = noise(own_keys[0], (MEMBERS, D), 1.0, 6.0, ((0, 64),))
    member_key = draw_member_key(jax.random.fold_in(jax.random.fold_in(key_of[3], part), 71), part)
    limit_index = jax.random.randint(own_keys[2], (1,), 0, LIMITS).astype(jnp.int32)
    return {"embeddings": embeddings, "member_key": member_key, "limit_index": limit_index}


label_stride = 268435456

def normalize(embeddings):
    values = embeddings.astype(jnp.float32)
    mean_square = lax.optimization_barrier(jnp.mean(values * values, axis=1, keepdims=True))
    scaled = values * lax.rsqrt(mean_square + 1e-06) * (1.0 / math.sqrt(values.shape[1]))
    return scaled.astype(jnp.bfloat16)

def reference(embeddings, member_key, limit_index):
    unit = normalize(embeddings)
    total = unit.shape[0]
    block_rows = math.gcd(total, 512)
    label_all = member_key // label_stride

    def one_block(index):
        begin = (index * block_rows).astype(jnp.int32)
        rows = lax.dynamic_slice_in_dim(unit, begin, block_rows, 0)
        keys = lax.dynamic_slice_in_dim(member_key, begin, block_rows, 0)
        labels = lax.dynamic_slice_in_dim(label_all, begin, block_rows, 0)
        scores = lax.dot_general(rows, unit, (((1,), (1,)), ((), ())), preferred_element_type=jnp.float32)
        allowed = (member_key[None, :] < keys[:, None]) & (label_all[None, :] == labels[:, None])
        return lax.optimization_barrier(jnp.max(jnp.where(allowed, scores, jnp.float32(-1.0)), axis=1))
    max_cosine = lax.map(one_block, jnp.arange(total // block_rows, dtype=jnp.int32)).reshape(total)
    width = math.sqrt(unit.shape[1])
    table = (2.0 + 0.5 * jnp.arange(LIMITS, dtype=jnp.float32)) / width
    limit = jnp.sum(jnp.where(jnp.arange(LIMITS, dtype=jnp.int32) == limit_index[0], table, jnp.float32(0.0)))
    kept = jax.nn.sigmoid(2.0 * width * (limit - max_cosine))
    kept_share = (jnp.sum(kept) / total).reshape(1)
    return (max_cosine, kept_share)
```

```python
import functools
import math

import jax
import jax.numpy as jnp
from jax import lax
from jax.experimental import pallas as pl
from jax.experimental.pallas import tpu as pltpu
from jax.sharding import PartitionSpec as P

LIMITS = 8
label_stride = 268435456
KEY_BASE = 32768
PIECES = 4


VMEM = pl.BlockSpec(memory_space=pltpu.VMEM)
PARAMS = pltpu.CompilerParams(vmem_limit_bytes=16 * 1024 * 1024)


def normalize_kernel(emb_ref, *out_refs):
    step = out_refs[0].shape[0]
    for n, out in enumerate(out_refs):
        values = emb_ref[n * step : (n + 1) * step, :].astype(jnp.float32)
        mean_square = jnp.mean(values * values, axis=1, keepdims=True)
        scaled = values * lax.rsqrt(mean_square + 1e-06) * (1.0 / math.sqrt(values.shape[1]))
        out[...] = scaled.astype(jnp.bfloat16)


def normalize(embeddings, pieces):
    rows, width = embeddings.shape
    out = jax.ShapeDtypeStruct((rows // pieces, width), jnp.bfloat16)
    return pl.pallas_call(
        normalize_kernel,
        out_shape=[out] * pieces,
        in_specs=[VMEM],
        out_specs=[VMEM] * pieces,
        compiler_params=PARAMS,
        cost_estimate=pl.CostEstimate(flops=rows * width * 4, bytes_accessed=rows * width * 4, transcendentals=rows),
        name="normalize",
    )(embeddings)


def whole_key(note):
    return note[0:1].astype(jnp.int32) * KEY_BASE + note[1:2].astype(jnp.int32)


def score_kernel(row_pieces, first_row, groups, *refs):
    note_ref, acc_ref = refs[0], refs[1]
    rows_refs = refs[2 : 2 + row_pieces]
    out_ref = refs[-1]
    rest = refs[2 + row_pieces : -1]
    rows = jnp.concatenate([r[...] for r in rows_refs], axis=0)
    count = rows.shape[0]
    row_key = whole_key(note_ref[...])[:, first_row : first_row + count]
    low = row_key & jnp.int32(-label_stride)
    best = acc_ref[...]
    at = 0
    for pieces in groups:
        other_note, piece_refs = rest[at], rest[at + 1 : at + 1 + len(pieces)]
        at += 1 + len(pieces)
        others = whole_key(other_note[...])
        total = others.shape[1]
        key_col = jnp.broadcast_to(others, (128, total)).T
        for index, ref in zip(pieces, piece_refs):
            size = ref.shape[0]
            scores = lax.dot_general(
                ref[...], rows, (((1,), (1,)), ((), ())), preferred_element_type=jnp.float32
            )
            key = key_col[index * size : (index + 1) * size, 0:1]
            allowed = (key < row_key) & (key >= low)
            best = jnp.maximum(
                best, jnp.max(jnp.where(allowed, scores, jnp.float32(-1.0)), axis=0, keepdims=True)
            )
    out_ref[...] = best


def score(note, acc, rows, first_row, groups):
    count = sum(r.shape[0] for r in rows)
    others = sum(p.shape[0] for _, ps in groups for _, p in ps)
    width = rows[0].shape[1]
    operands = [note, acc, *rows]
    for other_note, pieces in groups:
        operands += [other_note, *[p for _, p in pieces]]
    return pl.pallas_call(
        functools.partial(
            score_kernel, len(rows), first_row, [tuple(i for i, _ in ps) for _, ps in groups]
        ),
        out_shape=jax.ShapeDtypeStruct((1, count), jnp.float32),
        in_specs=[VMEM] * len(operands),
        out_specs=VMEM,
        compiler_params=PARAMS,
        cost_estimate=pl.CostEstimate(
            flops=2 * count * others * width,
            bytes_accessed=2 * (count + others) * width,
            transcendentals=0,
        ),
        name="score",
    )(*operands)


def finish_kernel(width, place_ref, limit_ref, mine_ref, theirs_ref, best_ref, share_ref):
    blocks, rows = mine_ref.shape
    half = rows // 2
    first, second, blk = place_ref[0], place_ref[1], place_ref[2]
    k = limit_ref[0]
    limit = jnp.float32(0.0)
    for entry in range(LIMITS):
        value = jnp.float32((2.0 + 0.5 * entry) / width)
        limit = jnp.where(k == entry, value, limit)
    total = jnp.zeros((1, rows), jnp.float32)
    mine_all = jnp.concatenate([mine_ref[...], mine_ref[...]], axis=0)
    quarter = blocks // 4
    up_mine, down_mine = mine_all[quarter : quarter + blocks], mine_all[blocks - quarter : 2 * blocks - quarter]
    theirs = theirs_ref[...]
    swapped = jnp.concatenate([theirs[:, half:], theirs[:, :half]], axis=1)
    swapped_all = jnp.concatenate([swapped, swapped], axis=0)
    up_theirs, down_theirs = swapped_all[quarter : quarter + blocks], swapped_all[blocks - quarter : 2 * blocks - quarter]
    core0 = first == 1
    best = jnp.where(
        core0, jnp.maximum(up_mine, down_theirs), jnp.maximum(down_mine, up_theirs)
    )
    kept = jax.nn.sigmoid(2.0 * width * (limit - best))
    total = jnp.sum(kept, axis=0, keepdims=True)
    total = jnp.sum(total, axis=1, keepdims=True)
    share_ref[...] = total / (blocks * rows)
    at = lax.broadcasted_iota(jnp.int32, best.shape, 0)
    own = jnp.max(jnp.where(at == blk, best, jnp.float32(-2.0)), axis=0, keepdims=True)
    best_ref[...] = own[:, :half]


def finish(place, limit_index, mine, theirs, width):
    blocks, rows = mine.shape
    smem = pl.BlockSpec(memory_space=pltpu.SMEM)
    return pl.pallas_call(
        functools.partial(finish_kernel, width),
        out_shape=[
            jax.ShapeDtypeStruct((1, rows // 2), jnp.float32),
            jax.ShapeDtypeStruct((1, 1), jnp.float32),
        ],
        in_specs=[smem, smem, VMEM, VMEM],
        out_specs=[VMEM, VMEM],
        compiler_params=PARAMS,
        name="finish",
    )(place, limit_index, mine, theirs)


def on_device(embeddings, member_key, limit_index):
    chips, cores = lax.axis_size("blk"), lax.axis_size("sub")
    width = embeddings.shape[1]
    hops = chips // 4
    onward = [(cores * c, cores * ((c + 1) % chips)) for c in range(chips)]
    onward += [(cores * c + 1, cores * ((c - 1) % chips) + 1) for c in range(chips)]
    swap = [(0, 1), (1, 0)]

    def forward(x):
        return lax.ppermute(x, ("blk", "sub"), onward)

    def across(x):
        return lax.ppermute(x, "sub", swap)

    half = PIECES // 2
    own_key = jnp.stack(
        [(member_key // KEY_BASE).astype(jnp.float32), (member_key % KEY_BASE).astype(jnp.float32)]
    )
    other_key = across(own_key)
    mine = normalize(embeddings, half)
    theirs = [across(m) for m in mine]
    own = [*mine, *theirs]
    note = jnp.concatenate([own_key, other_key], axis=1)
    size = own[0].shape[0]
    pair = 2 * size
    own_all = (note, list(enumerate(own)))
    start = jnp.full((1, pair), -1.0, jnp.float32)
    halves = range(PIECES // 2)

    acc = [score(note, start, own[2 * p : 2 * p + 2], p * pair, [own_all]) for p in halves]
    message = jnp.concatenate([note, jnp.concatenate(acc, axis=1)], axis=0)

    block = own
    own_note = note
    previous = None
    for h in range(1, hops + 1):
        block = [forward(b) for b in block]
        message = forward(message)
        note = message[:2]
        acc = [message[2:3, p * pair : (p + 1) * pair] for p in halves]
        groups = [own_all]
        facing = None
        if h >= hops // 2:
            facing = (across(note), list(enumerate([across(b) for b in block])))
        if h > hops // 2:
            groups.append(previous)
            groups.append(facing)
        previous = facing
        new = []
        for p in halves:
            a = acc[p]
            if h == hops:
                a = score(note, a, block[2 * p : 2 * p + 2], p * pair, groups[:2])
                a = score(note, a, block[2 * p : 2 * p + 2], p * pair, groups[2:])
            else:
                a = score(note, a, block[2 * p : 2 * p + 2], p * pair, groups)
            new.append(a)
        acc = jnp.concatenate(new, axis=1)
        message = jnp.concatenate([note, acc], axis=0)

    everyone = jnp.broadcast_to(acc, (chips, acc.shape[1]))
    gathered = lax.all_to_all(everyone, "blk", 0, 0, tiled=True)
    facing = across(gathered)
    core = lax.axis_index("sub")
    place = jnp.stack([jnp.where(core == 0, 1, 0), core, lax.axis_index("blk")]).astype(jnp.int32)
    best, share = finish(place, limit_index, gathered, facing, math.sqrt(width))
    return (best.reshape(-1), share.reshape(1))


def solution(mesh):
    in_specs = (P(("groups", "blk", "sub"), None), P(("groups", "blk", "sub")), P("groups"))
    out_specs = (P(("groups", "blk", "sub")), P("groups"))
    return jax.shard_map(
        on_device, mesh=mesh, in_specs=in_specs, out_specs=out_specs, check_vma=False
    )
```

```python
import functools
import math

import jax
import jax.numpy as jnp
from jax import lax
from jax.experimental import pallas as pl
from jax.experimental.pallas import tpu as pltpu
from jax.sharding import PartitionSpec as P


LIMITS = 8
label_stride = 268435456
KEY_BASE = 32768
PIECES = 4


VMEM = pl.BlockSpec(memory_space=pltpu.VMEM)
PARAMS = pltpu.CompilerParams(vmem_limit_bytes=16 * 1024 * 1024)


def normalize_kernel(emb_ref, *out_refs):
    step = out_refs[0].shape[0]
    for n, out in enumerate(out_refs):
        values = emb_ref[n * step : (n + 1) * step, :].astype(jnp.float32)
        mean_square = jnp.mean(values * values, axis=1, keepdims=True)
        scaled = values * lax.rsqrt(mean_square + 1e-06) * (1.0 / math.sqrt(values.shape[1]))
        out[...] = scaled.astype(jnp.bfloat16)


def normalize(embeddings, pieces):
    rows, width = embeddings.shape
    out = jax.ShapeDtypeStruct((rows // pieces, width), jnp.bfloat16)
    return pl.pallas_call(
        normalize_kernel,
        out_shape=[out] * pieces,
        in_specs=[VMEM],
        out_specs=[VMEM] * pieces,
        compiler_params=PARAMS,
        cost_estimate=pl.CostEstimate(flops=rows * width * 4, bytes_accessed=rows * width * 4, transcendentals=rows),
        name="normalize",
    )(embeddings)


def whole_key(note):
    return note[0:1].astype(jnp.int32) * KEY_BASE + note[1:2].astype(jnp.int32)


def key_columns(note):
    keys = whole_key(note)
    return jnp.broadcast_to(keys, (128, keys.shape[1])).T


def best_of(best, row_key, low, rows, others, key_col):
    scores = lax.dot_general(
        others, rows, (((1,), (1,)), ((), ())), preferred_element_type=jnp.float32
    )
    count = rows.shape[0]
    key = jnp.concatenate([key_col] * (-(-count // 128)), axis=1)[:, :count]
    allowed = (key < row_key) & (key >= low)
    masked = jnp.where(allowed, scores, jnp.float32(-1.0))
    return jnp.maximum(best, jnp.max(masked, axis=0, keepdims=True))


def lay_kernel(*refs):
    size = refs[0].shape[0]
    for n, ref in enumerate(refs[:-1]):
        refs[-1][n * size : (n + 1) * size, :] = ref[...]


def lay(pieces):
    rows, width = sum(p.shape[0] for p in pieces), pieces[0].shape[1]
    return pl.pallas_call(
        lay_kernel,
        out_shape=jax.ShapeDtypeStruct((rows, width), jnp.bfloat16),
        in_specs=[VMEM] * len(pieces),
        out_specs=VMEM,
        compiler_params=PARAMS,
        cost_estimate=pl.CostEstimate(flops=rows, bytes_accessed=4 * rows * width, transcendentals=0),
        name="lay",
    )(*pieces)


def visit_kernel(note_ref, whole_ref, *refs):
    best_ref, columns_ref = refs[-2:]
    note = note_ref[...]
    columns_ref[...] = key_columns(note)
    own_ref, own_columns_ref = refs[:2] if len(refs) > 2 else (whole_ref, columns_ref)
    row_key = whole_key(note)
    low = row_key & jnp.int32(-label_stride)
    rows = whole_ref[...]
    step = rows.shape[0] // 2

    def part(n, best):
        at = pl.ds(pl.multiple_of(n * step, step), step)
        return best_of(best, row_key, low, rows, own_ref[at, :], own_columns_ref[at, :])

    best_ref[...] = lax.fori_loop(0, 2, part, jnp.full(best_ref.shape, -1.0, jnp.float32))


def visit(note, whole, own):
    rows, width = whole.shape
    operands = [note, whole, *own]
    return pl.pallas_call(
        visit_kernel,
        out_shape=[
            jax.ShapeDtypeStruct((1, rows), jnp.float32),
            jax.ShapeDtypeStruct((rows, 128), jnp.int32),
        ],
        in_specs=[VMEM] * len(operands),
        out_specs=[VMEM] * 2,
        compiler_params=PARAMS,
        cost_estimate=pl.CostEstimate(
            flops=rows, bytes_accessed=6 * rows * width, transcendentals=0
        ),
        name="visit",
    )(*operands)


def meet_kernel(first_row, pieces, blocks, extra, spread, *refs):
    note_ref = refs[0]
    rows = jnp.concatenate([r[...] for r in refs[1 : 1 + pieces]], axis=0)
    at = 1 + pieces
    count = rows.shape[0]
    row_key = whole_key(note_ref[...])[:, first_row : first_row + count]
    low = row_key & jnp.int32(-label_stride)
    best = jnp.full((1, count), -1.0, jnp.float32)
    for _ in range(blocks):
        best = best_of(best, row_key, low, rows, refs[at][...], refs[at + 1][...])
        at += 2
    if extra:
        others = jnp.concatenate([r[...] for r in refs[at + 1 : at + 1 + extra]], axis=0)
        best = best_of(best, row_key, low, rows, others, key_columns(refs[at][...]))
        at += 1 + extra
    out_ref = refs[-1]
    if spread:
        earlier = refs[at][...]
        for ref in refs[at + 1 : -2]:
            earlier = jnp.maximum(earlier, ref[...])
        best = jnp.maximum(refs[-2][...], jnp.concatenate([earlier, best], axis=1))
        out_ref[...] = jnp.broadcast_to(best[:, None, :], out_ref.shape)
    else:
        out_ref[...] = best


def meet(note, first_row, pieces, blocks, extra=(), spread=(), chips=0):
    count, width = sum(p.shape[0] for p in pieces), pieces[0].shape[1]
    operands = [note, *pieces]
    for whole, columns in blocks:
        operands += [whole, columns]
    operands += [*extra, *spread]
    others = sum(whole.shape[0] for whole, _ in blocks) + sum(p.shape[0] for p in extra[1:])
    out = (chips, 1, note.shape[1]) if spread else (1, count)
    return pl.pallas_call(
        functools.partial(
            meet_kernel, first_row, len(pieces), len(blocks), max(len(extra) - 1, 0), bool(spread)
        ),
        out_shape=jax.ShapeDtypeStruct(out, jnp.float32),
        in_specs=[VMEM] * len(operands),
        out_specs=VMEM,
        compiler_params=PARAMS,
        cost_estimate=pl.CostEstimate(
            flops=2 * count * others * width,
            bytes_accessed=2 * (count + others) * width,
            transcendentals=0,
        ),
        name="meet",
    )(*operands)


def finish_kernel(width, place_ref, limit_ref, mine_ref, theirs_ref, best_ref, share_ref):
    blocks, rows = mine_ref.shape
    half = rows // 2
    core, blk = place_ref[0], place_ref[1]
    k = limit_ref[0]
    limit = jnp.float32(0.0)
    for entry in range(LIMITS):
        limit = jnp.where(k == entry, jnp.float32((2.0 + 0.5 * entry) / width), limit)
    quarter = blocks // 4

    def turned(x, by):
        return jnp.concatenate([x[by:], x[:by]], axis=0)

    mine, theirs = mine_ref[...], theirs_ref[...]
    mine = jnp.concatenate([mine[:, half:], mine[:, :half]], axis=1)
    up, down = quarter, blocks - quarter
    best = jnp.where(
        core == 0,
        jnp.maximum(turned(mine, down), turned(theirs, up)),
        jnp.maximum(turned(mine, up), turned(theirs, down)),
    )
    kept = jax.nn.sigmoid(2.0 * width * (limit - best))
    total = jnp.sum(jnp.sum(kept, axis=0, keepdims=True), axis=1, keepdims=True)
    share_ref[...] = total / (blocks * rows)
    at = lax.broadcasted_iota(jnp.int32, best.shape, 0)
    own = jnp.max(jnp.where(at == blk, best, jnp.float32(-2.0)), axis=0, keepdims=True)
    best_ref[...] = own[:, :half]


def finish(place, limit_index, mine, theirs, width):
    _, rows = mine.shape
    smem = pl.BlockSpec(memory_space=pltpu.SMEM)
    return pl.pallas_call(
        functools.partial(finish_kernel, width),
        out_shape=[
            jax.ShapeDtypeStruct((1, rows // 2), jnp.float32),
            jax.ShapeDtypeStruct((1, 1), jnp.float32),
        ],
        in_specs=[smem, smem, VMEM, VMEM],
        out_specs=[VMEM, VMEM],
        compiler_params=PARAMS,
        name="finish",
    )(place, limit_index, mine, theirs)


def program(embeddings, member_key, limit_index):
    chips, cores = lax.axis_size("blk"), lax.axis_size("sub")
    width = embeddings.shape[1]
    hops = chips // 4
    onward, crossing = [], []
    for c in range(chips):
        for core, to in ((0, (c + 1) % chips), (1, (c - 1) % chips)):
            onward.append((cores * c + core, cores * to + core))
            crossing.append((cores * c + core, cores * to + 1 - core))

    def forward(x, pairs=onward):
        return lax.ppermute(x, ("blk", "sub"), pairs)

    def carry(block, pairs=onward):
        moved = []
        for piece in block:
            moved.append(forward(piece, pairs))
        return moved

    def across(x):
        return lax.ppermute(x, "sub", [(0, 1), (1, 0)])

    half = PIECES // 2
    own_key = jnp.stack(
        [(member_key // KEY_BASE).astype(jnp.float32), (member_key % KEY_BASE).astype(jnp.float32)]
    )
    other_key = across(own_key)
    mine = normalize(embeddings, half)
    theirs = [across(m) for m in mine]
    block = [*mine, *theirs]
    note = jnp.concatenate([own_key, other_key], axis=1)
    whole = lay(block)
    best, columns = visit(note, whole, ())
    own = (whole, columns)
    held = [own]
    acc = best
    for _ in range(1, hops):
        block = carry(block)
        message = forward(jnp.concatenate([note, acc], axis=0))
        note = message[:2]
        whole = lay(block)
        best, columns = visit(note, whole, own)
        held.append((whole, columns))
        acc = jnp.maximum(message[2:3], best)
    block = carry(block, crossing)
    note = forward(note, crossing)
    acc = forward(acc, crossing)
    rows = note.shape[1] // 2
    first = lay(block[:half])
    facing = [across(note[:, :rows]), across(first)]
    early = [meet(note, 0, [first], held), meet(note, 0, [first], [], facing)]
    everyone = meet(note, rows, block[half:], held, facing, (*early, acc), chips)

    gathered = lax.all_to_all(everyone, "blk", 0, 0, tiled=True).reshape(chips, -1)
    other_side = across(gathered)
    place = jnp.stack([lax.axis_index("sub"), lax.axis_index("blk")]).astype(jnp.int32)
    best, share = finish(place, limit_index, gathered, other_side, math.sqrt(width))
    return (best.reshape(-1), share.reshape(1))


def solution(mesh):
    in_specs = (P(("groups", "blk", "sub"), None), P(("groups", "blk", "sub")), P("groups"))
    out_specs = (P(("groups", "blk", "sub")), P("groups"))
    return jax.shard_map(
        program, mesh=mesh, in_specs=in_specs, out_specs=out_specs, check_vma=False
    )
```

```python
import functools
import math

import jax
import jax.numpy as jnp
from jax import lax
from jax.experimental import pallas as pl
from jax.experimental.pallas import tpu as pltpu
from jax.sharding import PartitionSpec as P


LIMITS = 8
label_stride = 268435456
KEY_BASE = 32768
PIECES = 3


VMEM = pl.BlockSpec(memory_space=pltpu.VMEM)
PARAMS = pltpu.CompilerParams(vmem_limit_bytes=16 * 1024 * 1024)


def normalize_kernel(emb_ref, *out_refs):
    at = 0
    for out in out_refs:
        values = emb_ref[at : at + out.shape[0], :].astype(jnp.float32)
        mean_square = jnp.mean(values * values, axis=1, keepdims=True)
        scaled = values * lax.rsqrt(mean_square + 1e-06) * (1.0 / math.sqrt(values.shape[1]))
        out[...] = scaled.astype(jnp.bfloat16)
        at += out.shape[0]


def normalize(embeddings, sizes):
    rows, width = embeddings.shape
    return pl.pallas_call(
        normalize_kernel,
        out_shape=[jax.ShapeDtypeStruct((size, width), jnp.bfloat16) for size in sizes],
        in_specs=[VMEM],
        out_specs=[VMEM] * len(sizes),
        compiler_params=PARAMS,
        cost_estimate=pl.CostEstimate(
            flops=rows * width * 4, bytes_accessed=rows * width * 4, transcendentals=rows
        ),
        name="normalize",
    )(embeddings)


def whole_key(note):
    return note[0:1].astype(jnp.int32) * KEY_BASE + note[1:2].astype(jnp.int32)


def key_columns(note):
    keys = whole_key(note)
    return jnp.broadcast_to(keys, (128, keys.shape[1])).T


def best_of(best, row_key, low, rows, others, key_col):
    scores = lax.dot_general(
        others, rows, (((1,), (1,)), ((), ())), preferred_element_type=jnp.float32
    )
    count = rows.shape[0]
    key = jnp.concatenate([key_col] * (-(-count // 128)), axis=1)[:, :count]
    allowed = (key < row_key) & (key >= low)
    masked = jnp.where(allowed, scores, jnp.float32(-1.0))
    return jnp.maximum(best, jnp.max(masked, axis=0, keepdims=True))


def lay_kernel(count, starts, *refs):
    first = 0
    for ref in refs[:count]:
        end = first + ref.shape[0]
        for start, out in zip(starts, refs[count:]):
            low, high = max(first, start), min(end, start + out.shape[0])
            if low < high:
                out[low - start : high - start, :] = ref[low - first : high - first, :]
        first = end


def lay(pieces, cuts):
    width = pieces[0].shape[1]
    total = sum(end - start for start, end in cuts)
    return pl.pallas_call(
        functools.partial(lay_kernel, len(pieces), [start for start, _ in cuts]),
        out_shape=[jax.ShapeDtypeStruct((end - start, width), jnp.bfloat16) for start, end in cuts],
        in_specs=[VMEM] * len(pieces),
        out_specs=[VMEM] * len(cuts),
        compiler_params=PARAMS,
        cost_estimate=pl.CostEstimate(
            flops=total, bytes_accessed=4 * total * width, transcendentals=0
        ),
        name="lay",
    )(*pieces)


def visit_kernel(at_home, note_ref, whole_ref, own_note_ref, own_ref, own_columns_ref, *refs):
    best_ref, columns_ref = refs[-2:]
    note = note_ref[...]
    columns_ref[...] = key_columns(note)
    if at_home:
        key, rows_ref, others_ref, others_columns_ref = whole_key(own_note_ref[...]), own_ref, whole_ref, columns_ref
    else:
        key, rows_ref, others_ref, others_columns_ref = whole_key(note), whole_ref, own_ref, own_columns_ref
    low = key & jnp.int32(-label_stride)
    rows = rows_ref[...]
    step = rows.shape[0] // 2

    def part(n, best):
        at = pl.ds(pl.multiple_of(n * step, step), step)
        return best_of(best, key, low, rows, others_ref[at, :], others_columns_ref[at, :])

    start = refs[0][...] if len(refs) > 2 else jnp.full(best_ref.shape, -1.0, jnp.float32)
    best_ref[...] = lax.fori_loop(0, 2, part, start)


def visit(note, whole, own, acc=None):
    rows, width = whole.shape
    own_note, own_whole, own_columns = own
    operands = [note, whole, own_note, own_whole, own_columns]
    operands += [] if acc is None else [acc]
    return pl.pallas_call(
        functools.partial(visit_kernel, acc is not None),
        out_shape=[
            jax.ShapeDtypeStruct((1, rows), jnp.float32),
            jax.ShapeDtypeStruct((rows, 128), jnp.int32),
        ],
        in_specs=[VMEM] * len(operands),
        out_specs=[VMEM] * 2,
        compiler_params=PARAMS,
        cost_estimate=pl.CostEstimate(
            flops=rows, bytes_accessed=6 * rows * width, transcendentals=0
        ),
        name="visit",
    )(*operands)


def columns_kernel(note_ref, columns_ref):
    columns_ref[...] = key_columns(note_ref[...])


def columns_of(note):
    return pl.pallas_call(
        columns_kernel,
        out_shape=jax.ShapeDtypeStruct((note.shape[1], 128), jnp.int32),
        in_specs=[VMEM],
        out_specs=VMEM,
        compiler_params=PARAMS,
        name="columns",
    )(note)


def meet_kernel(first_row, pieces, blocks, extra, spread, *refs):
    note_ref = refs[0]
    rows = jnp.concatenate([r[...] for r in refs[1 : 1 + pieces]], axis=0)
    at = 1 + pieces
    count = rows.shape[0]
    row_key = whole_key(note_ref[...])[:, first_row : first_row + count]
    low = row_key & jnp.int32(-label_stride)
    best = jnp.full((1, count), -1.0, jnp.float32)
    for _ in range(blocks):
        best = best_of(best, row_key, low, rows, refs[at][...], refs[at + 1][...])
        at += 2
    if extra:
        others = jnp.concatenate([r[...] for r in refs[at + 1 : at + 1 + extra]], axis=0)
        best = best_of(best, row_key, low, rows, others, key_columns(refs[at][...]))
        at += 1 + extra
    out_ref = refs[-1]
    if spread:
        earlier = jnp.maximum(refs[at][...], refs[at + 1][...])
        best = jnp.concatenate([earlier, best], axis=1)
        for ref in refs[at + 2 : -1]:
            best = jnp.maximum(best, ref[...])
        out_ref[...] = jnp.broadcast_to(best[:, None, :], out_ref.shape)
    else:
        out_ref[...] = best


def meet(note, first_row, pieces, blocks, extra=(), spread=(), chips=0):
    count, width = sum(p.shape[0] for p in pieces), pieces[0].shape[1]
    operands = [note, *pieces]
    for whole, columns in blocks:
        operands += [whole, columns]
    operands += [*extra, *spread]
    others = sum(whole.shape[0] for whole, _ in blocks) + sum(p.shape[0] for p in extra[1:])
    out = (chips, 1, note.shape[1]) if spread else (1, count)
    return pl.pallas_call(
        functools.partial(
            meet_kernel, first_row, len(pieces), len(blocks), max(len(extra) - 1, 0), bool(spread)
        ),
        out_shape=jax.ShapeDtypeStruct(out, jnp.float32),
        in_specs=[VMEM] * len(operands),
        out_specs=VMEM,
        compiler_params=PARAMS,
        cost_estimate=pl.CostEstimate(
            flops=2 * count * others * width,
            bytes_accessed=2 * (count + others) * width,
            transcendentals=0,
        ),
        name="meet",
    )(*operands)


def finish_kernel(width, place_ref, limit_ref, mine_ref, theirs_ref, best_ref, share_ref):
    blocks, rows = mine_ref.shape
    half = rows // 2
    core, blk = place_ref[0], place_ref[1]
    k = limit_ref[0]
    limit = jnp.float32(0.0)
    for entry in range(LIMITS):
        limit = jnp.where(k == entry, jnp.float32((2.0 + 0.5 * entry) / width), limit)
    quarter = blocks // 4

    def turned(x, by):
        return jnp.concatenate([x[by:], x[:by]], axis=0)

    mine, theirs = mine_ref[...], theirs_ref[...]
    mine = jnp.concatenate([mine[:, half:], mine[:, :half]], axis=1)
    up, down = quarter, blocks - quarter
    best = jnp.where(
        core == 0,
        jnp.maximum(turned(mine, down), turned(theirs, up)),
        jnp.maximum(turned(mine, up), turned(theirs, down)),
    )
    kept = jax.nn.sigmoid(2.0 * width * (limit - best))
    total = jnp.sum(jnp.sum(kept, axis=0, keepdims=True), axis=1, keepdims=True)
    share_ref[...] = total / (blocks * rows)
    at = lax.broadcasted_iota(jnp.int32, best.shape, 0)
    own = jnp.max(jnp.where(at == blk, best, jnp.float32(-2.0)), axis=0, keepdims=True)
    best_ref[...] = own[:, :half]


def finish(place, limit_index, mine, theirs, width):
    _, rows = mine.shape
    smem = pl.BlockSpec(memory_space=pltpu.SMEM)
    return pl.pallas_call(
        functools.partial(finish_kernel, width),
        out_shape=[
            jax.ShapeDtypeStruct((1, rows // 2), jnp.float32),
            jax.ShapeDtypeStruct((1, 1), jnp.float32),
        ],
        in_specs=[smem, smem, VMEM, VMEM],
        out_specs=[VMEM, VMEM],
        compiler_params=PARAMS,
        name="finish",
    )(place, limit_index, mine, theirs)


def program(embeddings, member_key, limit_index):
    chips, cores = lax.axis_size("blk"), lax.axis_size("sub")
    rows, width = embeddings.shape
    hops = chips // 4

    def moves(by, change):
        pairs = []
        for c in range(chips):
            for core, to in ((0, (c + by) % chips), (1, (c - by) % chips)):
                pairs.append((cores * c + core, cores * to + (1 - core if change else core)))
        return pairs

    def send(x, by, change=False):
        return lax.ppermute(x, ("blk", "sub"), moves(by, change))

    def across(x):
        return lax.ppermute(x, "sub", [(0, 1), (1, 0)])

    size = cores * rows // PIECES
    cuts = [(n * size, (n + 1) * size) for n in range(PIECES)]
    everything = (0, cores * rows)
    own_key = jnp.stack(
        [(member_key // KEY_BASE).astype(jnp.float32), (member_key % KEY_BASE).astype(jnp.float32)]
    )
    mine = normalize(embeddings, (size, rows - size))
    theirs = [across(m) for m in mine]
    note = jnp.concatenate([own_key, across(own_key)], axis=1)
    *rest, whole = lay([*mine, *theirs], [*cuts[1:], everything])
    block = [mine[0], *rest]
    notes = [note]
    while len(notes) < hops:
        by = len(notes)
        far = send(jnp.concatenate(notes, axis=0), by)
        notes += [far[2 * n : 2 * n + 2] for n in range(by)]
    last_note = send(note, hops, True)
    own = (note, whole, columns_of(note))
    held = [own[1:]]
    start = jnp.full((1, cores * rows), -1.0, jnp.float32)
    acc, _ = visit(note, whole, own, start)
    for h in range(1, hops):
        block = [send(b, 1) for b in block]
        (whole,) = lay(block, [everything])
        if h < hops - 1:
            acc, columns = visit(notes[h], whole, own, acc)
        else:
            late, columns = visit(notes[h], whole, own)
        held.append((whole, columns))
    acc = send(acc, hops, True)
    late = send(late, 1, True)
    block = [send(b, 1, True) for b in block]
    (first,) = lay(block[:-1], [(0, rows)])
    facing = [across(last_note[:, :rows]), across(first)]
    split = size * (PIECES - 1)
    early = [meet(last_note, 0, block[:-1], held), meet(last_note, 0, block[:-1], [], facing)]
    everyone = meet(last_note, split, block[-1:], held, facing, (*early, acc, late), chips)

    gathered = lax.all_to_all(everyone, "blk", 0, 0, tiled=True).reshape(chips, -1)
    other_side = across(gathered)
    place = jnp.stack([lax.axis_index("sub"), lax.axis_index("blk")]).astype(jnp.int32)
    best, share = finish(place, limit_index, gathered, other_side, math.sqrt(width))
    return (best.reshape(-1), share.reshape(1))


def solution(mesh):
    in_specs = (P(("groups", "blk", "sub"), None), P(("groups", "blk", "sub")), P("groups"))
    out_specs = (P(("groups", "blk", "sub")), P("groups"))
    return jax.shard_map(
        program, mesh=mesh, in_specs=in_specs, out_specs=out_specs, check_vma=False
    )
```

```python
import functools
import math

import jax
import jax.numpy as jnp
from jax import lax
from jax.experimental import pallas as pl
from jax.experimental.pallas import tpu as pltpu
from jax.sharding import PartitionSpec as P


LIMITS = 8
label_stride = 268435456
TAIL = 8
PIECES = 3


VMEM = pl.BlockSpec(memory_space=pltpu.VMEM)
PARAMS = pltpu.CompilerParams(vmem_limit_bytes=16 * 1024 * 1024)


def normalize_kernel(emb_ref, *out_refs):
    at = 0
    for out in out_refs:
        values = emb_ref[at : at + out.shape[0], :].astype(jnp.float32)
        mean_square = jnp.mean(values * values, axis=1, keepdims=True)
        scaled = values * lax.rsqrt(mean_square + 1e-06) * (1.0 / math.sqrt(values.shape[1]))
        out[...] = scaled.astype(jnp.bfloat16)
        at += out.shape[0]


def normalize(embeddings, sizes):
    rows, width = embeddings.shape
    return pl.pallas_call(
        normalize_kernel,
        out_shape=[jax.ShapeDtypeStruct((size, width), jnp.bfloat16) for size in sizes],
        in_specs=[VMEM],
        out_specs=[VMEM] * len(sizes),
        compiler_params=PARAMS,
        cost_estimate=pl.CostEstimate(
            flops=rows * width * 4, bytes_accessed=rows * width * 4, transcendentals=rows
        ),
        name="normalize",
    )(embeddings)


def key_columns(keys):
    return jnp.broadcast_to(keys, (128, keys.shape[1])).T


def read_tail(ref, count):
    tail = ref[ref.shape[0] - TAIL :, :count].astype(jnp.float32)
    keys = jnp.zeros((1, count), jnp.int32)
    for n in range(4):
        keys = keys * 256 + tail[n : n + 1].astype(jnp.int32)
    return keys, tail[4:5] + tail[5:6] + tail[6:7]


def write_tail(ref, keys, acc):
    rows = [((keys >> (24 - 8 * n)) & 255).astype(jnp.float32) for n in range(4)]
    for _ in range(3):
        part = acc.astype(jnp.bfloat16).astype(jnp.float32)
        rows.append(part)
        acc = acc - part
    rows.append(jnp.zeros_like(acc))
    count, start = keys.shape[1], ref.shape[0] - TAIL
    ref[start:, :count] = jnp.concatenate(rows, axis=0).astype(jnp.bfloat16)
    ref[start:, count:] = jnp.zeros((TAIL, ref.shape[1] - count), jnp.bfloat16)


def best_of(best, row_key, low, rows, others, key_col):
    scores = lax.dot_general(
        others, rows, (((1,), (1,)), ((), ())), preferred_element_type=jnp.float32
    )
    count = rows.shape[0]
    key = jnp.concatenate([key_col] * (-(-count // 128)), axis=1)[:, :count]
    allowed = (key < row_key) & (key >= low)
    masked = jnp.where(allowed, scores, jnp.float32(-1.0))
    return jnp.maximum(best, jnp.max(masked, axis=0, keepdims=True))


def lay_kernel(count, starts, *refs):
    first = 0
    for ref in refs[:count]:
        end = first + ref.shape[0]
        for start, out in zip(starts, refs[count:]):
            low, high = max(first, start), min(end, start + out.shape[0])
            if low < high:
                out[low - start : high - start, :] = ref[low - first : high - first, :]
        first = end


def lay(pieces, cuts):
    width = pieces[0].shape[1]
    total = sum(end - start for start, end in cuts)
    return pl.pallas_call(
        functools.partial(lay_kernel, len(pieces), [start for start, _ in cuts]),
        out_shape=[jax.ShapeDtypeStruct((end - start, width), jnp.bfloat16) for start, end in cuts],
        in_specs=[VMEM] * len(pieces),
        out_specs=[VMEM] * len(cuts),
        compiler_params=PARAMS,
        cost_estimate=pl.CostEstimate(
            flops=total, bytes_accessed=4 * total * width, transcendentals=0
        ),
        name="lay",
    )(*pieces)


def front_visit_kernel(pieces, keys_ref, own_ref, own_columns_ref, *refs):
    best_ref, columns_ref = refs[-2:]
    keys = keys_ref[...]
    columns_ref[...] = key_columns(keys)
    rows = jnp.concatenate([r[...] for r in refs[:pieces]], axis=0)
    count = rows.shape[0]
    row_key = keys[:, :count]
    low = row_key & jnp.int32(-label_stride)
    start = jnp.full(best_ref.shape, -1.0, jnp.float32)
    best_ref[...] = best_of(start, row_key, low, rows, own_ref[...], own_columns_ref[...])


def front_visit(keys, own, pieces):
    total, width = own[0].shape
    count = sum(p.shape[0] for p in pieces)
    operands = [keys, *own, *pieces]
    return pl.pallas_call(
        functools.partial(front_visit_kernel, len(pieces)),
        out_shape=[
            jax.ShapeDtypeStruct((1, count), jnp.float32),
            jax.ShapeDtypeStruct((total, 128), jnp.int32),
        ],
        in_specs=[VMEM] * len(operands),
        out_specs=[VMEM] * 2,
        compiler_params=PARAMS,
        cost_estimate=pl.CostEstimate(
            flops=total, bytes_accessed=4 * total * width, transcendentals=0
        ),
        name="front_visit",
    )(*operands)


def last_visit_kernel(begins, keys_ref, own_ref, own_columns_ref, front_ref, piece_ref, *refs):
    if begins:
        next_ref, out_ref = refs
        earlier, next_keys = None, next_ref[...]
    else:
        next_out_ref, out_ref = refs
        next_keys, earlier = read_tail(piece_ref, keys_ref.shape[1])
        next_out_ref[...] = next_keys
    keys = keys_ref[...]
    count = out_ref.shape[0] - TAIL
    rows = piece_ref[:count, :]
    row_key = keys[:, keys.shape[1] - count :]
    low = row_key & jnp.int32(-label_stride)
    start = jnp.full((1, count), -1.0, jnp.float32)
    best = best_of(start, row_key, low, rows, own_ref[...], own_columns_ref[...])
    acc = jnp.concatenate([front_ref[...], best], axis=1)
    if earlier is not None:
        acc = jnp.maximum(acc, earlier)
    out_ref[:count, :] = rows
    write_tail(out_ref, next_keys, acc)


def last_visit(keys, own, front, piece, next_keys=None):
    begins = next_keys is not None
    total, width = own[0].shape
    rows = piece.shape[0] + (TAIL if begins else 0)
    operands = [keys, *own, front, piece] + ([next_keys] if begins else [])
    out_shape = [] if begins else [jax.ShapeDtypeStruct(keys.shape, jnp.int32)]
    out_shape.append(jax.ShapeDtypeStruct((rows, width), jnp.bfloat16))
    return pl.pallas_call(
        functools.partial(last_visit_kernel, begins),
        out_shape=out_shape,
        in_specs=[VMEM] * len(operands),
        out_specs=[VMEM] * len(out_shape),
        compiler_params=PARAMS,
        cost_estimate=pl.CostEstimate(
            flops=total, bytes_accessed=4 * total * width, transcendentals=0
        ),
        name="last_visit",
    )(*operands)


def columns_kernel(keys_ref, columns_ref):
    columns_ref[...] = key_columns(keys_ref[...])


def columns_of(keys):
    return pl.pallas_call(
        columns_kernel,
        out_shape=jax.ShapeDtypeStruct((keys.shape[1], 128), jnp.int32),
        in_specs=[VMEM],
        out_specs=VMEM,
        compiler_params=PARAMS,
        name="columns",
    )(keys)


def meet_kernel(first_row, pieces, blocks, extra, spread, *refs):
    note_ref = refs[0]
    count = min(sum(r.shape[0] for r in refs[1 : 1 + pieces]), note_ref.shape[1] - first_row)
    rows = jnp.concatenate([r[...] for r in refs[1 : 1 + pieces]], axis=0)[:count]
    at = 1 + pieces
    row_key = note_ref[:, first_row : first_row + count]
    low = row_key & jnp.int32(-label_stride)
    best = jnp.full((1, count), -1.0, jnp.float32)
    for _ in range(blocks):
        best = best_of(best, row_key, low, rows, refs[at][...], refs[at + 1][...])
        at += 2
    if extra:
        others = jnp.concatenate([r[...] for r in refs[at + 1 : at + 1 + extra]], axis=0)
        columns = key_columns(refs[at][...])[: others.shape[0]]
        best = best_of(best, row_key, low, rows, others, columns)
        at += 1 + extra
    out_ref = refs[-1]
    if spread:
        earlier = jnp.maximum(refs[at][...], refs[at + 1][...])
        best = jnp.concatenate([earlier, best], axis=1)
        best = jnp.maximum(best, read_tail(refs[1], best.shape[1])[1])
        out_ref[...] = jnp.broadcast_to(best[:, None, :], out_ref.shape)
    else:
        out_ref[...] = best


def meet(note, first_row, pieces, blocks, extra=(), spread=(), chips=0):
    count, width = sum(p.shape[0] for p in pieces), pieces[0].shape[1]
    operands = [note, *pieces]
    for whole, columns in blocks:
        operands += [whole, columns]
    operands += [*extra, *spread]
    others = sum(whole.shape[0] for whole, _ in blocks) + sum(p.shape[0] for p in extra[1:])
    out = (chips, 1, note.shape[1]) if spread else (1, count)
    return pl.pallas_call(
        functools.partial(
            meet_kernel, first_row, len(pieces), len(blocks), max(len(extra) - 1, 0), bool(spread)
        ),
        out_shape=jax.ShapeDtypeStruct(out, jnp.float32),
        in_specs=[VMEM] * len(operands),
        out_specs=VMEM,
        compiler_params=PARAMS,
        cost_estimate=pl.CostEstimate(
            flops=2 * count * others * width,
            bytes_accessed=2 * (count + others) * width,
            transcendentals=0,
        ),
        name="meet",
    )(*operands)


def finish_kernel(width, place_ref, limit_ref, mine_ref, theirs_ref, best_ref, share_ref):
    blocks, rows = mine_ref.shape
    half = rows // 2
    core, blk = place_ref[0], place_ref[1]
    k = limit_ref[0]
    limit = jnp.float32(0.0)
    for entry in range(LIMITS):
        limit = jnp.where(k == entry, jnp.float32((2.0 + 0.5 * entry) / width), limit)
    quarter = blocks // 4

    def turned(x, by):
        return jnp.concatenate([x[by:], x[:by]], axis=0)

    mine, theirs = mine_ref[...], theirs_ref[...]
    mine = jnp.concatenate([mine[:, half:], mine[:, :half]], axis=1)
    up, down = quarter, blocks - quarter
    best = jnp.where(
        core == 0,
        jnp.maximum(turned(mine, down), turned(theirs, up)),
        jnp.maximum(turned(mine, up), turned(theirs, down)),
    )
    kept = jax.nn.sigmoid(2.0 * width * (limit - best))
    total = jnp.sum(jnp.sum(kept, axis=0, keepdims=True), axis=1, keepdims=True)
    share_ref[...] = total / (blocks * rows)
    at = lax.broadcasted_iota(jnp.int32, best.shape, 0)
    own = jnp.max(jnp.where(at == blk, best, jnp.float32(-2.0)), axis=0, keepdims=True)
    best_ref[...] = own[:, :half]


def finish(place, limit_index, mine, theirs, width):
    _, rows = mine.shape
    smem = pl.BlockSpec(memory_space=pltpu.SMEM)
    return pl.pallas_call(
        functools.partial(finish_kernel, width),
        out_shape=[
            jax.ShapeDtypeStruct((1, rows // 2), jnp.float32),
            jax.ShapeDtypeStruct((1, 1), jnp.float32),
        ],
        in_specs=[smem, smem, VMEM, VMEM],
        out_specs=[VMEM, VMEM],
        compiler_params=PARAMS,
        name="finish",
    )(place, limit_index, mine, theirs)


def program(embeddings, member_key, limit_index):
    chips, cores = lax.axis_size("blk"), lax.axis_size("sub")
    rows, width = embeddings.shape
    hops = chips // 4

    def moves(by, change):
        pairs = []
        for c in range(chips):
            for core, to in ((0, (c + by) % chips), (1, (c - by) % chips)):
                pairs.append((cores * c + core, cores * to + (1 - core if change else core)))
        return pairs

    def send(x, by, change=False):
        return lax.ppermute(x, ("blk", "sub"), moves(by, change))

    def across(x):
        return lax.ppermute(x, "sub", [(0, 1), (1, 0)])

    total = cores * rows
    size = total // PIECES
    cuts = [(n * size, (n + 1) * size) for n in range(PIECES)]
    keys = member_key.reshape(1, rows)
    keys = jnp.concatenate([keys, across(keys)], axis=1)
    next_keys = send(keys, 1)
    mine = normalize(embeddings, (size, rows - size))
    theirs = [across(m) for m in mine]
    *rest, whole = lay([*mine, *theirs], [*cuts[1:], (0, total)])
    block = [mine[0], *rest]
    own = (whole, columns_of(keys))
    held = [own]
    best, _ = front_visit(keys, own, block[:-1])
    (block[-1],) = last_visit(keys, own, best, block[-1], next_keys)
    for _ in range(1, hops):
        keys = next_keys
        block = [send(b, 1) for b in block]
        best, columns = front_visit(keys, own, block[:-1])
        next_keys, last = last_visit(keys, own, best, block[-1])
        (whole,) = lay(block, [(0, total)])
        held.append((whole, columns))
        block[-1] = last
    last_keys = across(next_keys)
    block = [send(b, 1, True) for b in block]
    (first,) = lay(block[:-1], [(0, rows)])
    facing = [next_keys, across(first)]
    split = size * (PIECES - 1)
    early = [meet(last_keys, 0, block[:-1], held), meet(last_keys, 0, block[:-1], [], facing)]
    everyone = meet(last_keys, split, block[-1:], held, facing, early, chips)

    gathered = lax.all_to_all(everyone, "blk", 0, 0, tiled=True).reshape(chips, -1)
    other_side = across(gathered)
    place = jnp.stack([lax.axis_index("sub"), lax.axis_index("blk")]).astype(jnp.int32)
    best, share = finish(place, limit_index, gathered, other_side, math.sqrt(width))
    return (best.reshape(-1), share.reshape(1))


def solution(mesh):
    in_specs = (P(("groups", "blk", "sub"), None), P(("groups", "blk", "sub")), P("groups"))
    out_specs = (P(("groups", "blk", "sub")), P("groups"))
    return jax.shard_map(
        program, mesh=mesh, in_specs=in_specs, out_specs=out_specs, check_vma=False
    )
```

```python
import functools
import math

import jax
import jax.numpy as jnp
from jax import lax
from jax.experimental import pallas as pl
from jax.experimental.pallas import tpu as pltpu
from jax.sharding import PartitionSpec as P


LIMITS = 8
label_stride = 268435456
TAIL = 8
PIECES = 3


VMEM = pl.BlockSpec(memory_space=pltpu.VMEM)
PARAMS = pltpu.CompilerParams(vmem_limit_bytes=16 * 1024 * 1024)


def normalize_kernel(emb_ref, *out_refs):
    at = 0
    for out in out_refs:
        values = emb_ref[at : at + out.shape[0], :].astype(jnp.float32)
        mean_square = jnp.mean(values * values, axis=1, keepdims=True)
        scaled = values * lax.rsqrt(mean_square + 1e-06) * (1.0 / math.sqrt(values.shape[1]))
        out[...] = scaled.astype(jnp.bfloat16)
        at += out.shape[0]


def normalize(embeddings, sizes):
    rows, width = embeddings.shape
    return pl.pallas_call(
        normalize_kernel,
        out_shape=[jax.ShapeDtypeStruct((size, width), jnp.bfloat16) for size in sizes],
        in_specs=[VMEM],
        out_specs=[VMEM] * len(sizes),
        compiler_params=PARAMS,
        cost_estimate=pl.CostEstimate(
            flops=rows * width * 4, bytes_accessed=rows * width * 4, transcendentals=rows
        ),
        name="normalize",
    )(embeddings)


def key_columns(keys):
    return jnp.broadcast_to(keys, (128, keys.shape[1])).T


def read_tail(ref, count):
    tail = ref[ref.shape[0] - TAIL :, :count].astype(jnp.float32)
    keys = jnp.zeros((1, count), jnp.int32)
    for n in range(4):
        keys = keys * 256 + tail[n : n + 1].astype(jnp.int32)
    return keys, tail[4:5] + tail[5:6] + tail[6:7]


def write_tail(ref, keys, acc):
    rows = [((keys >> (24 - 8 * n)) & 255).astype(jnp.float32) for n in range(4)]
    for _ in range(3):
        part = acc.astype(jnp.bfloat16).astype(jnp.float32)
        rows.append(part)
        acc = acc - part
    rows.append(jnp.zeros_like(acc))
    count, start = keys.shape[1], ref.shape[0] - TAIL
    ref[start:, :count] = jnp.concatenate(rows, axis=0).astype(jnp.bfloat16)
    ref[start:, count:] = jnp.zeros((TAIL, ref.shape[1] - count), jnp.bfloat16)


def best_of(best, row_key, low, rows, others, key_col):
    scores = lax.dot_general(
        others, rows, (((1,), (1,)), ((), ())), preferred_element_type=jnp.float32
    )
    count = rows.shape[0]
    key = jnp.concatenate([key_col] * (-(-count // 128)), axis=1)[:, :count]
    allowed = (key < row_key) & (key >= low)
    masked = jnp.where(allowed, scores, jnp.float32(-1.0))
    return jnp.maximum(best, jnp.max(masked, axis=0, keepdims=True))


def lay_kernel(count, starts, keyed, *refs):
    first = 0
    if keyed:
        refs[-1][...] = key_columns(refs[count][...])
        refs = refs[:count] + refs[count + 1 : -1]
    for ref in refs[:count]:
        end = first + ref.shape[0]
        for start, out in zip(starts, refs[count:]):
            low, high = max(first, start), min(end, start + out.shape[0])
            if low < high:
                out[low - start : high - start, :] = ref[low - first : high - first, :]
        first = end


def lay(pieces, cuts, keys=()):
    width = pieces[0].shape[1]
    total = sum(end - start for start, end in cuts)
    return pl.pallas_call(
        functools.partial(lay_kernel, len(pieces), [start for start, _ in cuts], bool(keys)),
        out_shape=[jax.ShapeDtypeStruct((end - start, width), jnp.bfloat16) for start, end in cuts]
        + [jax.ShapeDtypeStruct((k.shape[1], 128), jnp.int32) for k in keys],
        in_specs=[VMEM] * (len(pieces) + len(keys)),
        out_specs=[VMEM] * (len(cuts) + len(keys)),
        compiler_params=PARAMS,
        cost_estimate=pl.CostEstimate(
            flops=total, bytes_accessed=4 * total * width, transcendentals=0
        ),
        name="lay",
    )(*pieces, *keys)


def visit_kernel(begins, pieces, own_ref, own_columns_ref, *refs):
    piece_refs, out_ref = refs[:pieces], refs[-1]
    count = out_ref.shape[0] - TAIL
    last = piece_refs[-1][:count, :]
    rows = jnp.concatenate([*[r[...] for r in piece_refs[:-1]], last], axis=0)
    acc = jnp.full((1, rows.shape[0]), -1.0, jnp.float32)
    if begins:
        keys = refs[pieces][...]
    else:
        keys, acc = read_tail(piece_refs[-1], rows.shape[0])
        refs[pieces][...] = keys
    low = keys & jnp.int32(-label_stride)
    acc = best_of(acc, keys, low, rows, own_ref[...], own_columns_ref[...])
    out_ref[:count, :] = last
    write_tail(out_ref, keys, acc)


def visit(own, pieces, keys=None):
    begins = keys is not None
    total, width = own[0].shape
    rows = pieces[-1].shape[0] + (TAIL if begins else 0)
    operands = [*own, *pieces] + ([keys] if begins else [])
    out_shape = [] if begins else [jax.ShapeDtypeStruct((1, total), jnp.int32)]
    out_shape.append(jax.ShapeDtypeStruct((rows, width), jnp.bfloat16))
    return pl.pallas_call(
        functools.partial(visit_kernel, begins, len(pieces)),
        out_shape=out_shape,
        in_specs=[VMEM] * len(operands),
        out_specs=[VMEM] * len(out_shape),
        compiler_params=PARAMS,
        cost_estimate=pl.CostEstimate(
            flops=total, bytes_accessed=4 * total * width, transcendentals=0
        ),
        name="visit",
    )(*operands)


def columns_kernel(keys_ref, columns_ref):
    columns_ref[...] = key_columns(keys_ref[...])


def columns_of(keys):
    return pl.pallas_call(
        columns_kernel,
        out_shape=jax.ShapeDtypeStruct((keys.shape[1], 128), jnp.int32),
        in_specs=[VMEM],
        out_specs=VMEM,
        compiler_params=PARAMS,
        name="columns",
    )(keys)


def meet_kernel(first_row, pieces, blocks, extra, spread, *refs):
    note_ref = refs[0]
    count = min(sum(r.shape[0] for r in refs[1 : 1 + pieces]), note_ref.shape[1] - first_row)
    rows = jnp.concatenate([r[...] for r in refs[1 : 1 + pieces]], axis=0)[:count]
    at = 1 + pieces
    row_key = note_ref[:, first_row : first_row + count]
    low = row_key & jnp.int32(-label_stride)
    best = jnp.full((1, count), -1.0, jnp.float32)
    for _ in range(blocks):
        best = best_of(best, row_key, low, rows, refs[at][...], refs[at + 1][...])
        at += 2
    if extra:
        others = jnp.concatenate([r[...] for r in refs[at + 1 : at + 1 + extra]], axis=0)
        columns = key_columns(refs[at][...])[: others.shape[0]]
        best = best_of(best, row_key, low, rows, others, columns)
        at += 1 + extra
    out_ref = refs[-1]
    if spread:
        earlier = jnp.maximum(refs[at][...], refs[at + 1][...])
        best = jnp.concatenate([earlier, best], axis=1)
        best = jnp.maximum(best, read_tail(refs[1], best.shape[1])[1])
        out_ref[...] = jnp.broadcast_to(best[:, None, :], out_ref.shape)
    else:
        out_ref[...] = best


def meet(note, first_row, pieces, blocks, extra=(), spread=(), chips=0):
    count, width = sum(p.shape[0] for p in pieces), pieces[0].shape[1]
    operands = [note, *pieces]
    for whole, columns in blocks:
        operands += [whole, columns]
    operands += [*extra, *spread]
    others = sum(whole.shape[0] for whole, _ in blocks) + sum(p.shape[0] for p in extra[1:])
    out = (chips, 1, note.shape[1]) if spread else (1, count)
    return pl.pallas_call(
        functools.partial(
            meet_kernel, first_row, len(pieces), len(blocks), max(len(extra) - 1, 0), bool(spread)
        ),
        out_shape=jax.ShapeDtypeStruct(out, jnp.float32),
        in_specs=[VMEM] * len(operands),
        out_specs=VMEM,
        compiler_params=PARAMS,
        cost_estimate=pl.CostEstimate(
            flops=2 * count * others * width,
            bytes_accessed=2 * (count + others) * width,
            transcendentals=0,
        ),
        name="meet",
    )(*operands)


def finish_kernel(width, place_ref, limit_ref, mine_ref, theirs_ref, best_ref, share_ref):
    blocks, rows = mine_ref.shape
    half = rows // 2
    core, blk = place_ref[0], place_ref[1]
    k = limit_ref[0]
    limit = jnp.float32(0.0)
    for entry in range(LIMITS):
        limit = jnp.where(k == entry, jnp.float32((2.0 + 0.5 * entry) / width), limit)
    quarter = blocks // 4

    def turned(x, by):
        return jnp.concatenate([x[by:], x[:by]], axis=0)

    mine, theirs = mine_ref[...], theirs_ref[...]
    mine = jnp.concatenate([mine[:, half:], mine[:, :half]], axis=1)
    up, down = quarter, blocks - quarter
    best = jnp.where(
        core == 0,
        jnp.maximum(turned(mine, down), turned(theirs, up)),
        jnp.maximum(turned(mine, up), turned(theirs, down)),
    )
    kept = jax.nn.sigmoid(2.0 * width * (limit - best))
    total = jnp.sum(jnp.sum(kept, axis=0, keepdims=True), axis=1, keepdims=True)
    share_ref[...] = total / (blocks * rows)
    at = lax.broadcasted_iota(jnp.int32, best.shape, 0)
    own = jnp.max(jnp.where(at == blk, best, jnp.float32(-2.0)), axis=0, keepdims=True)
    best_ref[...] = own[:, :half]


def finish(place, limit_index, mine, theirs, width):
    _, rows = mine.shape
    smem = pl.BlockSpec(memory_space=pltpu.SMEM)
    return pl.pallas_call(
        functools.partial(finish_kernel, width),
        out_shape=[
            jax.ShapeDtypeStruct((1, rows // 2), jnp.float32),
            jax.ShapeDtypeStruct((1, 1), jnp.float32),
        ],
        in_specs=[smem, smem, VMEM, VMEM],
        out_specs=[VMEM, VMEM],
        compiler_params=PARAMS,
        name="finish",
    )(place, limit_index, mine, theirs)


def program(embeddings, member_key, limit_index):
    chips, cores = lax.axis_size("blk"), lax.axis_size("sub")
    rows, width = embeddings.shape
    hops = chips // 4

    def moves(by, change):
        pairs = []
        for c in range(chips):
            for core, to in ((0, (c + by) % chips), (1, (c - by) % chips)):
                pairs.append((cores * c + core, cores * to + (1 - core if change else core)))
        return pairs

    def send(x, by, change=False):
        return lax.ppermute(x, ("blk", "sub"), moves(by, change))

    def across(x):
        return lax.ppermute(x, "sub", [(0, 1), (1, 0)])

    total = cores * rows
    size = total // PIECES
    cuts = [(n * size, (n + 1) * size) for n in range(PIECES)]
    keys = member_key.reshape(1, rows)
    keys = jnp.concatenate([keys, across(keys)], axis=1)
    mine = normalize(embeddings, (size, rows - size))
    theirs = [across(m) for m in mine]
    (second,) = lay([mine[1], theirs[0]], [(0, size)])
    *rest, whole = lay([*mine, *theirs], [*cuts[2:], (0, total)])
    block = [mine[0], second, *rest]
    own = (whole, columns_of(keys))
    held = [own]
    (block[-1],) = visit(own, block, keys)
    for _ in range(1, hops):
        block = [send(b, 1) for b in block]
        keys, last = visit(own, block)
        held.append(lay(block, [(0, total)], [keys]))
        block[-1] = last
    last_keys = send(keys, 1, True)
    next_keys = send(keys, 1)
    block = [send(b, 1, True) for b in block]
    (first,) = lay(block[:-1], [(0, rows)])
    facing = [next_keys, across(first)]
    split = size * (PIECES - 1)
    early = [meet(last_keys, 0, block[:-1], held), meet(last_keys, 0, block[:-1], [], facing)]
    everyone = meet(last_keys, split, block[-1:], held, facing, early, chips)

    gathered = lax.all_to_all(everyone, "blk", 0, 0, tiled=True).reshape(chips, -1)
    other_side = across(gathered)
    place = jnp.stack([lax.axis_index("sub"), lax.axis_index("blk")]).astype(jnp.int32)
    best, share = finish(place, limit_index, gathered, other_side, math.sqrt(width))
    return (best.reshape(-1), share.reshape(1))


def solution(mesh):
    in_specs = (P(("groups", "blk", "sub"), None), P(("groups", "blk", "sub")), P("groups"))
    out_specs = (P(("groups", "blk", "sub")), P("groups"))
    return jax.shard_map(
        program, mesh=mesh, in_specs=in_specs, out_specs=out_specs, check_vma=False
    )
```

```python
import functools
import math

import jax
import jax.numpy as jnp
from jax import lax
from jax.experimental import pallas as pl
from jax.experimental.pallas import tpu as pltpu
from jax.sharding import PartitionSpec as P


LIMITS = 8
label_stride = 268435456
TAIL = 8
PIECES = 3


VMEM = pl.BlockSpec(memory_space=pltpu.VMEM)
PARAMS = pltpu.CompilerParams(vmem_limit_bytes=16 * 1024 * 1024)


def normalize_kernel(emb_ref, *out_refs):
    at = 0
    for out in out_refs:
        values = emb_ref[at : at + out.shape[0], :].astype(jnp.float32)
        mean_square = jnp.mean(values * values, axis=1, keepdims=True)
        scaled = values * lax.rsqrt(mean_square + 1e-06) * (1.0 / math.sqrt(values.shape[1]))
        out[...] = scaled.astype(jnp.bfloat16)
        at += out.shape[0]


def normalize(embeddings, sizes):
    rows, width = embeddings.shape
    return pl.pallas_call(
        normalize_kernel,
        out_shape=[jax.ShapeDtypeStruct((size, width), jnp.bfloat16) for size in sizes],
        in_specs=[VMEM],
        out_specs=[VMEM] * len(sizes),
        compiler_params=PARAMS,
        cost_estimate=pl.CostEstimate(
            flops=rows * width * 4, bytes_accessed=rows * width * 4, transcendentals=rows
        ),
        name="normalize",
    )(embeddings)


def key_columns(keys):
    return jnp.broadcast_to(keys, (128, keys.shape[1])).T


def read_tail(ref, count):
    tail = ref[ref.shape[0] - TAIL :, :count].astype(jnp.float32)
    keys = jnp.zeros((1, count), jnp.int32)
    for n in range(4):
        keys = keys * 256 + tail[n : n + 1].astype(jnp.int32)
    return keys, tail[4:5] + tail[5:6] + tail[6:7]


def write_tail(ref, keys, acc):
    rows = [((keys >> (24 - 8 * n)) & 255).astype(jnp.float32) for n in range(4)]
    for _ in range(3):
        part = acc.astype(jnp.bfloat16).astype(jnp.float32)
        rows.append(part)
        acc = acc - part
    rows.append(jnp.zeros_like(acc))
    count, start = keys.shape[1], ref.shape[0] - TAIL
    ref[start:, :count] = jnp.concatenate(rows, axis=0).astype(jnp.bfloat16)
    ref[start:, count:] = jnp.zeros((TAIL, ref.shape[1] - count), jnp.bfloat16)


def best_of(best, row_key, low, rows, others, key_col):
    scores = lax.dot_general(
        others, rows, (((1,), (1,)), ((), ())), preferred_element_type=jnp.float32
    )
    count = rows.shape[0]
    key = jnp.concatenate([key_col] * (-(-count // 128)), axis=1)[:, :count]
    allowed = (key < row_key) & (key >= low)
    masked = jnp.where(allowed, scores, jnp.float32(-1.0))
    return jnp.maximum(best, jnp.max(masked, axis=0, keepdims=True))


def lay_kernel(count, starts, keyed, *refs):
    first = 0
    if keyed:
        refs[-1][...] = key_columns(refs[count][...])
        refs = refs[:count] + refs[count + 1 : -1]
    for ref in refs[:count]:
        end = first + ref.shape[0]
        for start, out in zip(starts, refs[count:]):
            low, high = max(first, start), min(end, start + out.shape[0])
            if low < high:
                out[low - start : high - start, :] = ref[low - first : high - first, :]
        first = end


def lay(pieces, cuts, keys=()):
    width = pieces[0].shape[1]
    total = sum(end - start for start, end in cuts)
    return pl.pallas_call(
        functools.partial(lay_kernel, len(pieces), [start for start, _ in cuts], bool(keys)),
        out_shape=[jax.ShapeDtypeStruct((end - start, width), jnp.bfloat16) for start, end in cuts]
        + [jax.ShapeDtypeStruct((k.shape[1], 128), jnp.int32) for k in keys],
        in_specs=[VMEM] * (len(pieces) + len(keys)),
        out_specs=[VMEM] * (len(cuts) + len(keys)),
        compiler_params=PARAMS,
        cost_estimate=pl.CostEstimate(
            flops=total, bytes_accessed=4 * total * width, transcendentals=0
        ),
        name="lay",
    )(*pieces, *keys)


def visit_kernel(begins, pieces, own_ref, own_columns_ref, *refs):
    piece_refs, out_ref = refs[:pieces], refs[-1]
    count = out_ref.shape[0] - TAIL
    last = piece_refs[-1][:count, :]
    rows = jnp.concatenate([*[r[...] for r in piece_refs[:-1]], last], axis=0)
    acc = jnp.full((1, rows.shape[0]), -1.0, jnp.float32)
    if begins:
        keys = refs[pieces][...]
    else:
        keys, acc = read_tail(piece_refs[-1], rows.shape[0])
        refs[pieces][...] = keys
    low = keys & jnp.int32(-label_stride)
    acc = best_of(acc, keys, low, rows, own_ref[...], own_columns_ref[...])
    out_ref[:count, :] = last
    write_tail(out_ref, keys, acc)


def visit(own, pieces, keys=None):
    begins = keys is not None
    total, width = own[0].shape
    rows = pieces[-1].shape[0] + (TAIL if begins else 0)
    operands = [*own, *pieces] + ([keys] if begins else [])
    out_shape = [] if begins else [jax.ShapeDtypeStruct((1, total), jnp.int32)]
    out_shape.append(jax.ShapeDtypeStruct((rows, width), jnp.bfloat16))
    return pl.pallas_call(
        functools.partial(visit_kernel, begins, len(pieces)),
        out_shape=out_shape,
        in_specs=[VMEM] * len(operands),
        out_specs=[VMEM] * len(out_shape),
        compiler_params=PARAMS,
        cost_estimate=pl.CostEstimate(
            flops=total, bytes_accessed=4 * total * width, transcendentals=0
        ),
        name="visit",
    )(*operands)


def late_visit_kernel(pieces, own_ref, own_columns_ref, *refs):
    piece_refs, out_ref = refs[:pieces], refs[-1]
    total = out_ref.shape[1]
    rows = jnp.concatenate([r[...] for r in piece_refs], axis=0)[:total]
    keys, acc = read_tail(piece_refs[-1], total)
    low = keys & jnp.int32(-label_stride)
    out_ref[...] = best_of(acc, keys, low, rows, own_ref[...], own_columns_ref[...])


def late_visit(own, pieces):
    total, width = own[0].shape
    operands = [*own, *pieces]
    return pl.pallas_call(
        functools.partial(late_visit_kernel, len(pieces)),
        out_shape=jax.ShapeDtypeStruct((1, total), jnp.float32),
        in_specs=[VMEM] * len(operands),
        out_specs=VMEM,
        compiler_params=PARAMS,
        cost_estimate=pl.CostEstimate(
            flops=total, bytes_accessed=4 * total * width, transcendentals=0
        ),
        name="late_visit",
    )(*operands)


def decode_kernel(piece_ref, keys_ref):
    keys_ref[...] = read_tail(piece_ref, keys_ref.shape[1])[0]


def decode(piece, count):
    return pl.pallas_call(
        decode_kernel,
        out_shape=jax.ShapeDtypeStruct((1, count), jnp.int32),
        in_specs=[VMEM],
        out_specs=VMEM,
        compiler_params=PARAMS,
        name="decode",
    )(piece)


def columns_kernel(keys_ref, columns_ref):
    columns_ref[...] = key_columns(keys_ref[...])


def columns_of(keys):
    return pl.pallas_call(
        columns_kernel,
        out_shape=jax.ShapeDtypeStruct((keys.shape[1], 128), jnp.int32),
        in_specs=[VMEM],
        out_specs=VMEM,
        compiler_params=PARAMS,
        name="columns",
    )(keys)


def meet_kernel(first_row, pieces, blocks, extra, spread, *refs):
    note_ref = refs[0]
    count = min(sum(r.shape[0] for r in refs[1 : 1 + pieces]), note_ref.shape[1] - first_row)
    rows = jnp.concatenate([r[...] for r in refs[1 : 1 + pieces]], axis=0)[:count]
    at = 1 + pieces
    row_key = note_ref[:, first_row : first_row + count]
    low = row_key & jnp.int32(-label_stride)
    best = jnp.full((1, count), -1.0, jnp.float32)
    for _ in range(blocks):
        best = best_of(best, row_key, low, rows, refs[at][...], refs[at + 1][...])
        at += 2
    if extra:
        others = jnp.concatenate([r[...] for r in refs[at + 1 : at + 1 + extra]], axis=0)
        columns = key_columns(refs[at][...])[: others.shape[0]]
        best = best_of(best, row_key, low, rows, others, columns)
        at += 1 + extra
    out_ref = refs[-1]
    if spread:
        earlier = jnp.maximum(refs[at][...], refs[at + 1][...])
        best = jnp.concatenate([earlier, best], axis=1)
        best = jnp.maximum(best, read_tail(refs[1], best.shape[1])[1])
        best = jnp.maximum(best, refs[at + 2][...])
        out_ref[...] = jnp.broadcast_to(best[:, None, :], out_ref.shape)
    else:
        out_ref[...] = best


def meet(note, first_row, pieces, blocks, extra=(), spread=(), chips=0):
    count, width = sum(p.shape[0] for p in pieces), pieces[0].shape[1]
    operands = [note, *pieces]
    for whole, columns in blocks:
        operands += [whole, columns]
    operands += [*extra, *spread]
    others = sum(whole.shape[0] for whole, _ in blocks) + sum(p.shape[0] for p in extra[1:])
    out = (chips, 1, note.shape[1]) if spread else (1, count)
    return pl.pallas_call(
        functools.partial(
            meet_kernel, first_row, len(pieces), len(blocks), max(len(extra) - 1, 0), bool(spread)
        ),
        out_shape=jax.ShapeDtypeStruct(out, jnp.float32),
        in_specs=[VMEM] * len(operands),
        out_specs=VMEM,
        compiler_params=PARAMS,
        cost_estimate=pl.CostEstimate(
            flops=2 * count * others * width,
            bytes_accessed=2 * (count + others) * width,
            transcendentals=0,
        ),
        name="meet",
    )(*operands)


def finish_kernel(width, place_ref, limit_ref, mine_ref, theirs_ref, best_ref, share_ref):
    blocks, rows = mine_ref.shape
    half = rows // 2
    core, blk = place_ref[0], place_ref[1]
    k = limit_ref[0]
    limit = jnp.float32(0.0)
    for entry in range(LIMITS):
        limit = jnp.where(k == entry, jnp.float32((2.0 + 0.5 * entry) / width), limit)
    quarter = blocks // 4

    def turned(x, by):
        return jnp.concatenate([x[by:], x[:by]], axis=0)

    mine, theirs = mine_ref[...], theirs_ref[...]
    mine = jnp.concatenate([mine[:, half:], mine[:, :half]], axis=1)
    up, down = quarter, blocks - quarter
    best = jnp.where(
        core == 0,
        jnp.maximum(turned(mine, down), turned(theirs, up)),
        jnp.maximum(turned(mine, up), turned(theirs, down)),
    )
    kept = jax.nn.sigmoid(2.0 * width * (limit - best))
    total = jnp.sum(jnp.sum(kept, axis=0, keepdims=True), axis=1, keepdims=True)
    share_ref[...] = total / (blocks * rows)
    at = lax.broadcasted_iota(jnp.int32, best.shape, 0)
    own = jnp.max(jnp.where(at == blk, best, jnp.float32(-2.0)), axis=0, keepdims=True)
    best_ref[...] = own[:, :half]


def finish(place, limit_index, mine, theirs, width):
    _, rows = mine.shape
    smem = pl.BlockSpec(memory_space=pltpu.SMEM)
    return pl.pallas_call(
        functools.partial(finish_kernel, width),
        out_shape=[
            jax.ShapeDtypeStruct((1, rows // 2), jnp.float32),
            jax.ShapeDtypeStruct((1, 1), jnp.float32),
        ],
        in_specs=[smem, smem, VMEM, VMEM],
        out_specs=[VMEM, VMEM],
        compiler_params=PARAMS,
        name="finish",
    )(place, limit_index, mine, theirs)


def program(embeddings, member_key, limit_index):
    chips, cores = lax.axis_size("blk"), lax.axis_size("sub")
    rows, width = embeddings.shape
    hops = chips // 4

    def moves(by, change):
        pairs = []
        for c in range(chips):
            for core, to in ((0, (c + by) % chips), (1, (c - by) % chips)):
                pairs.append((cores * c + core, cores * to + (1 - core if change else core)))
        return pairs

    def send(x, by, change=False):
        return lax.ppermute(x, ("blk", "sub"), moves(by, change))

    def across(x):
        return lax.ppermute(x, "sub", [(0, 1), (1, 0)])

    total = cores * rows
    size = total // PIECES
    cuts = [(n * size, (n + 1) * size) for n in range(PIECES)]
    keys = member_key.reshape(1, rows)
    keys = jnp.concatenate([keys, across(keys)], axis=1)
    mine = normalize(embeddings, (size, rows - size))
    theirs = [across(m) for m in mine]
    (second,) = lay([mine[1], theirs[0]], [(0, size)])
    *rest, whole = lay([*mine, *theirs], [*cuts[2:], (0, total)])
    block = [mine[0], second, *rest]
    own = (whole, columns_of(keys))
    held = [own]
    (block[-1],) = visit(own, block, keys)
    for h in range(1, hops):
        block = [send(b, 1) for b in block]
        if h < hops - 1:
            keys, last = visit(own, block)
        else:
            keys, last = decode(block[-1], total), block[-1]
            late = late_visit(own, block)
        held.append(lay(block, [(0, total)], [keys]))
        block[-1] = last
    last_keys = send(keys, 1, True)
    next_keys = send(keys, 1)
    late = send(late, 1, True)
    block = [send(b, 1, True) for b in block]
    (first,) = lay(block[:-1], [(0, rows)])
    facing = [next_keys, across(first)]
    split = size * (PIECES - 1)
    early = [meet(last_keys, 0, block[:-1], held), meet(last_keys, 0, block[:-1], [], facing)]
    everyone = meet(last_keys, split, block[-1:], held, facing, (*early, late), chips)

    gathered = lax.all_to_all(everyone, "blk", 0, 0, tiled=True).reshape(chips, -1)
    other_side = across(gathered)
    place = jnp.stack([lax.axis_index("sub"), lax.axis_index("blk")]).astype(jnp.int32)
    best, share = finish(place, limit_index, gathered, other_side, math.sqrt(width))
    return (best.reshape(-1), share.reshape(1))


def solution(mesh):
    in_specs = (P(("groups", "blk", "sub"), None), P(("groups", "blk", "sub")), P("groups"))
    out_specs = (P(("groups", "blk", "sub")), P("groups"))
    return jax.shard_map(
        program, mesh=mesh, in_specs=in_specs, out_specs=out_specs, check_vma=False
    )
```

```python
import functools
import math

import jax
import jax.numpy as jnp
from jax import lax
from jax.experimental import pallas as pl
from jax.experimental.pallas import tpu as pltpu
from jax.sharding import PartitionSpec as P


LIMITS = 8
label_stride = 268435456
TAIL = 8
PIECES = 3


VMEM = pl.BlockSpec(memory_space=pltpu.VMEM)
PARAMS = pltpu.CompilerParams(vmem_limit_bytes=16 * 1024 * 1024)


def normalize_kernel(emb_ref, *out_refs):
    at = 0
    for out in out_refs:
        values = emb_ref[at : at + out.shape[0], :].astype(jnp.float32)
        mean_square = jnp.mean(values * values, axis=1, keepdims=True)
        scaled = values * lax.rsqrt(mean_square + 1e-06) * (1.0 / math.sqrt(values.shape[1]))
        out[...] = scaled.astype(jnp.bfloat16)
        at += out.shape[0]


def normalize(embeddings, sizes):
    rows, width = embeddings.shape
    return pl.pallas_call(
        normalize_kernel,
        out_shape=[jax.ShapeDtypeStruct((size, width), jnp.bfloat16) for size in sizes],
        in_specs=[VMEM],
        out_specs=[VMEM] * len(sizes),
        compiler_params=PARAMS,
        cost_estimate=pl.CostEstimate(
            flops=rows * width * 4, bytes_accessed=rows * width * 4, transcendentals=rows
        ),
        name="normalize",
    )(embeddings)


def key_columns(keys):
    return jnp.broadcast_to(keys, (128, keys.shape[1])).T


def read_tail(ref, count):
    tail = ref[ref.shape[0] - TAIL :, :count].astype(jnp.float32)
    keys = jnp.zeros((1, count), jnp.int32)
    for n in range(4):
        keys = keys * 256 + tail[n : n + 1].astype(jnp.int32)
    return keys, tail[4:5] + tail[5:6] + tail[6:7]


def write_tail(ref, keys, acc):
    rows = [((keys >> (24 - 8 * n)) & 255).astype(jnp.float32) for n in range(4)]
    for _ in range(3):
        part = acc.astype(jnp.bfloat16).astype(jnp.float32)
        rows.append(part)
        acc = acc - part
    rows.append(jnp.zeros_like(acc))
    count, start = keys.shape[1], ref.shape[0] - TAIL
    ref[start:, :count] = jnp.concatenate(rows, axis=0).astype(jnp.bfloat16)
    ref[start:, count:] = jnp.zeros((TAIL, ref.shape[1] - count), jnp.bfloat16)


def best_of(best, row_key, low, rows, others, key_col):
    scores = lax.dot_general(
        others, rows, (((1,), (1,)), ((), ())), preferred_element_type=jnp.float32
    )
    count = rows.shape[0]
    key = jnp.concatenate([key_col] * (-(-count // 128)), axis=1)[:, :count]
    allowed = (key < row_key) & (key >= low)
    masked = jnp.where(allowed, scores, jnp.float32(-1.0))
    return jnp.maximum(best, jnp.max(masked, axis=0, keepdims=True))


def lay_kernel(count, starts, keyed, *refs):
    first = 0
    if keyed:
        refs[-1][...] = key_columns(refs[count][...])
        refs = refs[:count] + refs[count + 1 : -1]
    for ref in refs[:count]:
        end = first + ref.shape[0]
        for start, out in zip(starts, refs[count:]):
            low, high = max(first, start), min(end, start + out.shape[0])
            if low < high:
                out[low - start : high - start, :] = ref[low - first : high - first, :]
        first = end


def lay(pieces, cuts, keys=()):
    width = pieces[0].shape[1]
    total = sum(end - start for start, end in cuts)
    return pl.pallas_call(
        functools.partial(lay_kernel, len(pieces), [start for start, _ in cuts], bool(keys)),
        out_shape=[jax.ShapeDtypeStruct((end - start, width), jnp.bfloat16) for start, end in cuts]
        + [jax.ShapeDtypeStruct((k.shape[1], 128), jnp.int32) for k in keys],
        in_specs=[VMEM] * (len(pieces) + len(keys)),
        out_specs=[VMEM] * (len(cuts) + len(keys)),
        compiler_params=PARAMS,
        cost_estimate=pl.CostEstimate(
            flops=total, bytes_accessed=4 * total * width, transcendentals=0
        ),
        name="lay",
    )(*pieces, *keys)


def visit_kernel(begins, pieces, own_ref, own_columns_ref, *refs):
    piece_refs, out_ref = refs[:pieces], refs[-1]
    count = out_ref.shape[0] - TAIL
    last = piece_refs[-1][:count, :]
    rows = jnp.concatenate([*[r[...] for r in piece_refs[:-1]], last], axis=0)
    acc = jnp.full((1, rows.shape[0]), -1.0, jnp.float32)
    if begins:
        keys = refs[pieces][...]
    else:
        keys, acc = read_tail(piece_refs[-1], rows.shape[0])
        refs[pieces][...] = keys
    low = keys & jnp.int32(-label_stride)
    acc = best_of(acc, keys, low, rows, own_ref[...], own_columns_ref[...])
    out_ref[:count, :] = last
    write_tail(out_ref, keys, acc)


def visit(own, pieces, keys=None):
    begins = keys is not None
    total, width = own[0].shape
    rows = pieces[-1].shape[0] + (TAIL if begins else 0)
    operands = [*own, *pieces] + ([keys] if begins else [])
    out_shape = [] if begins else [jax.ShapeDtypeStruct((1, total), jnp.int32)]
    out_shape.append(jax.ShapeDtypeStruct((rows, width), jnp.bfloat16))
    return pl.pallas_call(
        functools.partial(visit_kernel, begins, len(pieces)),
        out_shape=out_shape,
        in_specs=[VMEM] * len(operands),
        out_specs=[VMEM] * len(out_shape),
        compiler_params=PARAMS,
        cost_estimate=pl.CostEstimate(
            flops=total, bytes_accessed=4 * total * width, transcendentals=0
        ),
        name="visit",
    )(*operands)


def late_visit_kernel(pieces, own_ref, own_columns_ref, *refs):
    piece_refs, out_ref = refs[:pieces], refs[-1]
    total = out_ref.shape[1]
    rows = jnp.concatenate([r[...] for r in piece_refs], axis=0)[:total]
    keys, acc = read_tail(piece_refs[-1], total)
    low = keys & jnp.int32(-label_stride)
    out_ref[...] = best_of(acc, keys, low, rows, own_ref[...], own_columns_ref[...])


def late_visit(own, pieces):
    total, width = own[0].shape
    operands = [*own, *pieces]
    return pl.pallas_call(
        functools.partial(late_visit_kernel, len(pieces)),
        out_shape=jax.ShapeDtypeStruct((1, total), jnp.float32),
        in_specs=[VMEM] * len(operands),
        out_specs=VMEM,
        compiler_params=PARAMS,
        cost_estimate=pl.CostEstimate(
            flops=total, bytes_accessed=4 * total * width, transcendentals=0
        ),
        name="late_visit",
    )(*operands)


def decode_kernel(piece_ref, keys_ref):
    keys_ref[...] = read_tail(piece_ref, keys_ref.shape[1])[0]


def decode(piece, count):
    return pl.pallas_call(
        decode_kernel,
        out_shape=jax.ShapeDtypeStruct((1, count), jnp.int32),
        in_specs=[VMEM],
        out_specs=VMEM,
        compiler_params=PARAMS,
        name="decode",
    )(piece)


def columns_kernel(keys_ref, columns_ref):
    columns_ref[...] = key_columns(keys_ref[...])


def columns_of(keys):
    return pl.pallas_call(
        columns_kernel,
        out_shape=jax.ShapeDtypeStruct((keys.shape[1], 128), jnp.int32),
        in_specs=[VMEM],
        out_specs=VMEM,
        compiler_params=PARAMS,
        name="columns",
    )(keys)


def meet_kernel(first_row, pieces, keys_ref, *refs):
    out_ref = refs[-1]
    count = out_ref.shape[1]
    rows = jnp.concatenate([r[...] for r in refs[:pieces]], axis=0)[:count]
    row_key = keys_ref[:, first_row : first_row + count]
    low = row_key & jnp.int32(-label_stride)
    best = jnp.full((1, count), -1.0, jnp.float32)
    for at in range(pieces, len(refs) - 1, 2):
        best = best_of(best, row_key, low, rows, refs[at][...], refs[at + 1][...])
    out_ref[...] = best


def meet(keys, first_row, count, pieces, blocks):
    width = pieces[0].shape[1]
    operands = [keys, *pieces]
    for whole, columns in blocks:
        operands += [whole, columns]
    others = sum(whole.shape[0] for whole, _ in blocks)
    return pl.pallas_call(
        functools.partial(meet_kernel, first_row, len(pieces)),
        out_shape=jax.ShapeDtypeStruct((1, count), jnp.float32),
        in_specs=[VMEM] * len(operands),
        out_specs=VMEM,
        compiler_params=PARAMS,
        cost_estimate=pl.CostEstimate(
            flops=2 * count * others * width,
            bytes_accessed=2 * (count + others) * width,
            transcendentals=0,
        ),
        name="meet",
    )(*operands)


def join_kernel(pieces, keys_ref, facing_keys_ref, facing_ref, late_ref, front_ref, back_ref, *refs):
    out_ref = refs[-1]
    keys = keys_ref[...]
    rows = jnp.concatenate([r[...] for r in refs[:pieces]], axis=0)[: keys.shape[1]]
    low = keys & jnp.int32(-label_stride)
    columns = key_columns(facing_keys_ref[...])[: facing_ref.shape[0]]
    best = jnp.concatenate([front_ref[...], back_ref[...]], axis=1)
    best = jnp.maximum(best, late_ref[...])
    best = best_of(best, keys, low, rows, facing_ref[...], columns)
    out_ref[...] = jnp.broadcast_to(best[:, None, :], out_ref.shape)


def join(keys, facing_keys, facing, late, front, back, pieces, chips):
    total = keys.shape[1]
    operands = [keys, facing_keys, facing, late, front, back, *pieces]
    return pl.pallas_call(
        functools.partial(join_kernel, len(pieces)),
        out_shape=jax.ShapeDtypeStruct((chips, 1, total), jnp.float32),
        in_specs=[VMEM] * len(operands),
        out_specs=VMEM,
        compiler_params=PARAMS,
        name="join",
    )(*operands)


def limit_kernel(root, index_ref, limit_ref):
    limit = jnp.zeros(limit_ref.shape, jnp.float32)
    for entry in range(LIMITS):
        value = jnp.float32((2.0 + 0.5 * entry) / root)
        limit = jnp.where(index_ref[0] == entry, value, limit)
    limit_ref[...] = limit


def limit_of(limit_index, root):
    return pl.pallas_call(
        functools.partial(limit_kernel, root),
        out_shape=jax.ShapeDtypeStruct((1, 128), jnp.float32),
        in_specs=[pl.BlockSpec(memory_space=pltpu.SMEM)],
        out_specs=VMEM,
        compiler_params=PARAMS,
        name="limit",
    )(limit_index)


def finish_kernel(width, limit_ref, mine_ref, theirs_ref, best_ref, share_ref):
    blocks, rows = mine_ref.shape
    half = rows // 2
    core, blk = lax.axis_index("sub"), lax.axis_index("blk")
    limit = limit_ref[:, :1]
    quarter = blocks // 4

    def turned(x, by):
        return jnp.concatenate([x[by:], x[:by]], axis=0)

    mine, theirs = mine_ref[...], theirs_ref[...]
    mine = jnp.concatenate([mine[:, half:], mine[:, :half]], axis=1)
    up, down = quarter, blocks - quarter
    best = jnp.where(
        core == 0,
        jnp.maximum(turned(mine, down), turned(theirs, up)),
        jnp.maximum(turned(mine, up), turned(theirs, down)),
    )
    kept = jax.nn.sigmoid(2.0 * width * (limit - best))
    total = jnp.sum(jnp.sum(kept, axis=0, keepdims=True), axis=1, keepdims=True)
    share_ref[...] = total / (blocks * rows)
    at = lax.broadcasted_iota(jnp.int32, best.shape, 0)
    own = jnp.max(jnp.where(at == blk, best, jnp.float32(-2.0)), axis=0, keepdims=True)
    best_ref[...] = own[:, :half]


def finish(limit, mine, theirs, width):
    rows = mine.shape[1]
    return pl.pallas_call(
        functools.partial(finish_kernel, width),
        out_shape=[
            jax.ShapeDtypeStruct((1, rows // 2), jnp.float32),
            jax.ShapeDtypeStruct((1, 1), jnp.float32),
        ],
        in_specs=[VMEM] * 3,
        out_specs=[VMEM, VMEM],
        compiler_params=PARAMS,
        name="finish",
    )(limit, mine, theirs)


def program(embeddings, member_key, limit_index):
    chips, cores = lax.axis_size("blk"), lax.axis_size("sub")
    rows, width = embeddings.shape
    hops = chips // 4

    def moves(by, change):
        pairs = []
        for c in range(chips):
            for core, to in ((0, (c + by) % chips), (1, (c - by) % chips)):
                pairs.append((cores * c + core, cores * to + (1 - core if change else core)))
        return pairs

    def send(x, by, change=False):
        return lax.ppermute(x, ("blk", "sub"), moves(by, change))

    def across(x):
        return lax.ppermute(x, "sub", [(0, 1), (1, 0)])

    total = cores * rows
    size = total // PIECES
    cuts = [(n * size, (n + 1) * size) for n in range(PIECES)]
    keys = member_key.reshape(1, rows)
    keys = jnp.concatenate([keys, across(keys)], axis=1)
    mine = normalize(embeddings, (size, rows - size))
    theirs = [across(m) for m in mine]
    (second,) = lay([mine[1], theirs[0]], [(0, size)])
    *rest, whole = lay([*mine, *theirs], [*cuts[2:], (0, total)])
    block = [mine[0], second, *rest]
    own = (whole, columns_of(keys))
    held = [own]
    (block[-1],) = visit(own, block, keys)
    for h in range(1, hops):
        block = [send(b, 1) for b in block]
        if h < hops - 1:
            keys, last = visit(own, block)
        else:
            keys, last = decode(block[-1], total), block[-1]
            late = late_visit(own, block)
        held.append(lay(block, [(0, total)], [keys]))
        block[-1] = last
    last_keys = send(keys, 1, True)
    next_keys = send(keys, 1)
    late = send(late, 1, True)
    block = [send(b, 1, True) for b in block]
    (first,) = lay(block[:-1], [(0, rows)])
    split = size * (PIECES - 1)
    front = meet(last_keys, 0, split, block[:-1], held)
    first, front = lax.optimization_barrier((first, front))
    facing = across(first)
    back = meet(last_keys, split, size, block[-1:], held)
    everyone = join(last_keys, next_keys, facing, late, front, back, block, chips)

    limit = limit_of(limit_index, math.sqrt(width))
    gathered = lax.all_to_all(everyone, "blk", 0, 0, tiled=True).reshape(chips, -1)
    other_side = across(gathered)
    root = math.sqrt(width)
    best, share = finish(limit, gathered, other_side, root)
    return (best.reshape(-1), share.reshape(1))


def solution(mesh):
    in_specs = (P(("groups", "blk", "sub"), None), P(("groups", "blk", "sub")), P("groups"))
    out_specs = (P(("groups", "blk", "sub")), P("groups"))
    return jax.shard_map(
        program, mesh=mesh, in_specs=in_specs, out_specs=out_specs, check_vma=False
    )
```

```python
import functools
import math

import jax
import jax.numpy as jnp
from jax import lax
from jax.experimental import pallas as pl
from jax.experimental.pallas import tpu as pltpu
from jax.sharding import PartitionSpec as P


LIMITS = 8
label_stride = 268435456
TAIL = 8
PIECES = 3


VMEM = pl.BlockSpec(memory_space=pltpu.VMEM)
PARAMS = pltpu.CompilerParams(vmem_limit_bytes=16 * 1024 * 1024)


def normalize_kernel(emb_ref, *out_refs):
    at = 0
    for out in out_refs:
        values = emb_ref[at : at + out.shape[0], :].astype(jnp.float32)
        mean_square = jnp.mean(values * values, axis=1, keepdims=True)
        scaled = values * lax.rsqrt(mean_square + 1e-06) * (1.0 / math.sqrt(values.shape[1]))
        out[...] = scaled.astype(jnp.bfloat16)
        at += out.shape[0]


def normalize(embeddings, sizes):
    rows, width = embeddings.shape
    return pl.pallas_call(
        normalize_kernel,
        out_shape=[jax.ShapeDtypeStruct((size, width), jnp.bfloat16) for size in sizes],
        in_specs=[VMEM],
        out_specs=[VMEM] * len(sizes),
        compiler_params=PARAMS,
        cost_estimate=pl.CostEstimate(
            flops=rows * width * 4, bytes_accessed=rows * width * 4, transcendentals=rows
        ),
        name="normalize",
    )(embeddings)


def key_columns(keys):
    return jnp.broadcast_to(keys, (128, keys.shape[1])).T


def read_tail(ref, count):
    tail = ref[ref.shape[0] - TAIL :, :count].astype(jnp.float32)
    keys = jnp.zeros((1, count), jnp.int32)
    for n in range(4):
        keys = keys * 256 + tail[n : n + 1].astype(jnp.int32)
    return keys, tail[4:5] + tail[5:6] + tail[6:7]


def write_tail(ref, keys, acc):
    rows = [((keys >> (24 - 8 * n)) & 255).astype(jnp.float32) for n in range(4)]
    for _ in range(3):
        part = acc.astype(jnp.bfloat16).astype(jnp.float32)
        rows.append(part)
        acc = acc - part
    rows.append(jnp.zeros_like(acc))
    count, start = keys.shape[1], ref.shape[0] - TAIL
    ref[start:, :count] = jnp.concatenate(rows, axis=0).astype(jnp.bfloat16)
    ref[start:, count:] = jnp.zeros((TAIL, ref.shape[1] - count), jnp.bfloat16)


def best_of(best, row_key, low, rows, others, key_col):
    scores = lax.dot_general(
        others, rows, (((1,), (1,)), ((), ())), preferred_element_type=jnp.float32
    )
    count = rows.shape[0]
    key = jnp.concatenate([key_col] * (-(-count // 128)), axis=1)[:, :count]
    allowed = (key < row_key) & (key >= low)
    masked = jnp.where(allowed, scores, jnp.float32(-1.0))
    return jnp.maximum(best, jnp.max(masked, axis=0, keepdims=True))


def lay_kernel(count, starts, keyed, *refs):
    first = 0
    if keyed:
        refs[-1][...] = key_columns(refs[count][...])
        refs = refs[:count] + refs[count + 1 : -1]
    for ref in refs[:count]:
        end = first + ref.shape[0]
        for start, out in zip(starts, refs[count:]):
            low, high = max(first, start), min(end, start + out.shape[0])
            if low < high:
                out[low - start : high - start, :] = ref[low - first : high - first, :]
        first = end


def lay(pieces, cuts, keys=()):
    width = pieces[0].shape[1]
    total = sum(end - start for start, end in cuts)
    return pl.pallas_call(
        functools.partial(lay_kernel, len(pieces), [start for start, _ in cuts], bool(keys)),
        out_shape=[jax.ShapeDtypeStruct((end - start, width), jnp.bfloat16) for start, end in cuts]
        + [jax.ShapeDtypeStruct((k.shape[1], 128), jnp.int32) for k in keys],
        in_specs=[VMEM] * (len(pieces) + len(keys)),
        out_specs=[VMEM] * (len(cuts) + len(keys)),
        compiler_params=PARAMS,
        cost_estimate=pl.CostEstimate(
            flops=total, bytes_accessed=4 * total * width, transcendentals=0
        ),
        name="lay",
    )(*pieces, *keys)


def visit_kernel(begins, pieces, own_ref, own_columns_ref, *refs):
    piece_refs, out_ref = refs[:pieces], refs[-1]
    count = out_ref.shape[0] - TAIL
    last = piece_refs[-1][:count, :]
    rows = jnp.concatenate([*[r[...] for r in piece_refs[:-1]], last], axis=0)
    acc = jnp.full((1, rows.shape[0]), -1.0, jnp.float32)
    if begins:
        keys = refs[pieces][...]
    else:
        keys, acc = read_tail(piece_refs[-1], rows.shape[0])
        refs[pieces][...] = keys
    low = keys & jnp.int32(-label_stride)
    acc = best_of(acc, keys, low, rows, own_ref[...], own_columns_ref[...])
    out_ref[:count, :] = last
    write_tail(out_ref, keys, acc)


def visit(own, pieces, keys=None):
    begins = keys is not None
    total, width = own[0].shape
    rows = pieces[-1].shape[0] + (TAIL if begins else 0)
    operands = [*own, *pieces] + ([keys] if begins else [])
    out_shape = [] if begins else [jax.ShapeDtypeStruct((1, total), jnp.int32)]
    out_shape.append(jax.ShapeDtypeStruct((rows, width), jnp.bfloat16))
    return pl.pallas_call(
        functools.partial(visit_kernel, begins, len(pieces)),
        out_shape=out_shape,
        in_specs=[VMEM] * len(operands),
        out_specs=[VMEM] * len(out_shape),
        compiler_params=PARAMS,
        cost_estimate=pl.CostEstimate(
            flops=total, bytes_accessed=4 * total * width, transcendentals=0
        ),
        name="visit",
    )(*operands)


def columns_kernel(keys_ref, columns_ref):
    columns_ref[...] = key_columns(keys_ref[...])


def columns_of(keys):
    return pl.pallas_call(
        columns_kernel,
        out_shape=jax.ShapeDtypeStruct((keys.shape[1], 128), jnp.int32),
        in_specs=[VMEM],
        out_specs=VMEM,
        compiler_params=PARAMS,
        name="columns",
    )(keys)


def meet_kernel(first_row, pieces, keys_ref, *refs):
    out_ref = refs[-1]
    count = out_ref.shape[1]
    rows = jnp.concatenate([r[...] for r in refs[:pieces]], axis=0)[:count]
    row_key = keys_ref[:, first_row : first_row + count]
    low = row_key & jnp.int32(-label_stride)
    best = jnp.full((1, count), -1.0, jnp.float32)
    for at in range(pieces, len(refs) - 1, 2):
        best = best_of(best, row_key, low, rows, refs[at][...], refs[at + 1][...])
    out_ref[...] = best


def meet(keys, first_row, count, pieces, blocks):
    width = pieces[0].shape[1]
    operands = [keys, *pieces]
    for whole, columns in blocks:
        operands += [whole, columns]
    others = sum(whole.shape[0] for whole, _ in blocks)
    return pl.pallas_call(
        functools.partial(meet_kernel, first_row, len(pieces)),
        out_shape=jax.ShapeDtypeStruct((1, count), jnp.float32),
        in_specs=[VMEM] * len(operands),
        out_specs=VMEM,
        compiler_params=PARAMS,
        cost_estimate=pl.CostEstimate(
            flops=2 * count * others * width,
            bytes_accessed=2 * (count + others) * width,
            transcendentals=0,
        ),
        name="meet",
    )(*operands)


def join_kernel(pieces, keys_ref, facing_keys_ref, facing_ref, front_ref, back_ref, *refs):
    out_ref = refs[-1]
    keys = keys_ref[...]
    rows = jnp.concatenate([r[...] for r in refs[:pieces]], axis=0)[: keys.shape[1]]
    low = keys & jnp.int32(-label_stride)
    columns = key_columns(facing_keys_ref[...])[: facing_ref.shape[0]]
    best = jnp.concatenate([front_ref[...], back_ref[...]], axis=1)
    best = jnp.maximum(best, read_tail(refs[pieces - 1], best.shape[1])[1])
    best = best_of(best, keys, low, rows, facing_ref[...], columns)
    out_ref[...] = jnp.broadcast_to(best[:, None, :], out_ref.shape)


def join(keys, facing_keys, facing, front, back, pieces, chips):
    total = keys.shape[1]
    operands = [keys, facing_keys, facing, front, back, *pieces]
    return pl.pallas_call(
        functools.partial(join_kernel, len(pieces)),
        out_shape=jax.ShapeDtypeStruct((chips, 1, total), jnp.float32),
        in_specs=[VMEM] * len(operands),
        out_specs=VMEM,
        compiler_params=PARAMS,
        name="join",
    )(*operands)


def limit_kernel(root, index_ref, limit_ref):
    limit = jnp.zeros(limit_ref.shape, jnp.float32)
    for entry in range(LIMITS):
        value = jnp.float32((2.0 + 0.5 * entry) / root)
        limit = jnp.where(index_ref[0] == entry, value, limit)
    limit_ref[...] = limit


def limit_of(limit_index, root):
    return pl.pallas_call(
        functools.partial(limit_kernel, root),
        out_shape=jax.ShapeDtypeStruct((1, 128), jnp.float32),
        in_specs=[pl.BlockSpec(memory_space=pltpu.SMEM)],
        out_specs=VMEM,
        compiler_params=PARAMS,
        name="limit",
    )(limit_index)


def finish_kernel(width, limit_ref, mine_ref, theirs_ref, best_ref, share_ref):
    blocks, rows = mine_ref.shape
    half = rows // 2
    core, blk = lax.axis_index("sub"), lax.axis_index("blk")
    limit = limit_ref[:, :1]
    quarter = blocks // 4

    def turned(x, by):
        return jnp.concatenate([x[by:], x[:by]], axis=0)

    mine, theirs = mine_ref[...], theirs_ref[...]
    mine = jnp.concatenate([mine[:, half:], mine[:, :half]], axis=1)
    up, down = quarter, blocks - quarter
    best = jnp.where(
        core == 0,
        jnp.maximum(turned(mine, down), turned(theirs, up)),
        jnp.maximum(turned(mine, up), turned(theirs, down)),
    )
    kept = jax.nn.sigmoid(2.0 * width * (limit - best))
    total = jnp.sum(jnp.sum(kept, axis=0, keepdims=True), axis=1, keepdims=True)
    share_ref[...] = total / (blocks * rows)
    at = lax.broadcasted_iota(jnp.int32, best.shape, 0)
    own = jnp.max(jnp.where(at == blk, best, jnp.float32(-2.0)), axis=0, keepdims=True)
    best_ref[...] = own[:, :half]


def finish(limit, mine, theirs, width):
    rows = mine.shape[1]
    return pl.pallas_call(
        functools.partial(finish_kernel, width),
        out_shape=[
            jax.ShapeDtypeStruct((1, rows // 2), jnp.float32),
            jax.ShapeDtypeStruct((1, 1), jnp.float32),
        ],
        in_specs=[VMEM] * 3,
        out_specs=[VMEM, VMEM],
        compiler_params=PARAMS,
        name="finish",
    )(limit, mine, theirs)


def program(embeddings, member_key, limit_index):
    chips, cores = lax.axis_size("blk"), lax.axis_size("sub")
    rows, width = embeddings.shape
    hops = chips // 4

    def moves(by, change):
        pairs = []
        for c in range(chips):
            for core, to in ((0, (c + by) % chips), (1, (c - by) % chips)):
                pairs.append((cores * c + core, cores * to + (1 - core if change else core)))
        return pairs

    def send(x, by, change=False):
        return lax.ppermute(x, ("blk", "sub"), moves(by, change))

    def across(x):
        return lax.ppermute(x, "sub", [(0, 1), (1, 0)])

    total = cores * rows
    size = total // PIECES
    cuts = [(n * size, (n + 1) * size) for n in range(PIECES)]
    keys = member_key.reshape(1, rows)
    keys = jnp.concatenate([keys, across(keys)], axis=1)
    mine = normalize(embeddings, (size, rows - size))
    theirs = [across(m) for m in mine]
    (second,) = lay([mine[1], theirs[0]], [(0, size)])
    *rest, whole = lay([*mine, *theirs], [*cuts[2:], (0, total)])
    block = [mine[0], second, *rest]
    own = (whole, columns_of(keys))
    held = [own]
    (block[-1],) = visit(own, block, keys)
    for _ in range(1, hops):
        block = [send(b, 1) for b in block]
        keys, last = visit(own, block)
        held.append(lay(block, [(0, total)], [keys]))
        block[-1] = last
    last_keys = send(keys, 1, True)
    next_keys = send(keys, 1)
    block = [send(b, 1, True) for b in block]
    (first,) = lay(block[:-1], [(0, rows)])
    split = size * (PIECES - 1)
    front = meet(last_keys, 0, split, block[:-1], held)
    first, front = lax.optimization_barrier((first, front))
    facing = across(first)
    back = meet(last_keys, split, size, block[-1:], held)
    everyone = join(last_keys, next_keys, facing, front, back, block, chips)

    limit = limit_of(limit_index, math.sqrt(width))
    gathered = lax.all_to_all(everyone, "blk", 0, 0, tiled=True).reshape(chips, -1)
    other_side = across(gathered)
    root = math.sqrt(width)
    best, share = finish(limit, gathered, other_side, root)
    return (best.reshape(-1), share.reshape(1))


def solution(mesh):
    in_specs = (P(("groups", "blk", "sub"), None), P(("groups", "blk", "sub")), P("groups"))
    out_specs = (P(("groups", "blk", "sub")), P("groups"))
    return jax.shard_map(
        program, mesh=mesh, in_specs=in_specs, out_specs=out_specs, check_vma=False
    )
```

```python
import functools
import math

import jax
import jax.numpy as jnp
from jax import lax
from jax.experimental import pallas as pl
from jax.experimental.pallas import tpu as pltpu
from jax.sharding import PartitionSpec as P


LIMITS = 8
label_stride = 268435456
TAIL = 8
PIECES = 3


VMEM = pl.BlockSpec(memory_space=pltpu.VMEM)
PARAMS = pltpu.CompilerParams(vmem_limit_bytes=16 * 1024 * 1024)


def normalize_kernel(emb_ref, *refs):
    held, arrived = refs[-2:]
    out_refs = refs[:-2]
    part = held.shape[1]
    copies = [
        pltpu.make_async_copy(emb_ref.at[pl.ds(n * part, part)], held.at[n], arrived.at[n])
        for n in range(held.shape[0])
    ]
    for copy in copies:
        copy.start()
    n = 0
    for out in out_refs:
        for at in range(0, out.shape[0], part):
            copies[n].wait()
            values = held[n].astype(jnp.float32)
            mean_square = jnp.mean(values * values, axis=1, keepdims=True)
            scaled = values * lax.rsqrt(mean_square + 1e-06) * (1.0 / math.sqrt(values.shape[1]))
            out[at : at + part, :] = scaled.astype(jnp.bfloat16)
            n += 1


def normalize(embeddings, sizes):
    rows, width = embeddings.shape
    part = math.gcd(*sizes) // 2
    return pl.pallas_call(
        normalize_kernel,
        out_shape=[jax.ShapeDtypeStruct((size, width), jnp.bfloat16) for size in sizes],
        in_specs=[pl.BlockSpec(memory_space=pltpu.HBM)],
        out_specs=[VMEM] * len(sizes),
        scratch_shapes=[
            pltpu.VMEM((rows // part, part, width), embeddings.dtype),
            pltpu.SemaphoreType.DMA((rows // part,)),
        ],
        compiler_params=pltpu.CompilerParams(vmem_limit_bytes=63 * 1024 * 1024 + 300 * 1024),
        cost_estimate=pl.CostEstimate(
            flops=rows * width * 4, bytes_accessed=rows * width * 4, transcendentals=rows
        ),
        name="normalize",
    )(embeddings)


def key_columns(keys):
    return jnp.broadcast_to(keys, (128, keys.shape[1])).T


def read_tail(ref, count):
    tail = ref[ref.shape[0] - TAIL :, :count].astype(jnp.float32)
    keys = jnp.zeros((1, count), jnp.int32)
    for n in range(4):
        keys = keys * 256 + tail[n : n + 1].astype(jnp.int32)
    return keys, tail[4:5] + tail[5:6] + tail[6:7]


def write_tail(ref, keys, acc):
    rows = [((keys >> (24 - 8 * n)) & 255).astype(jnp.float32) for n in range(4)]
    for _ in range(3):
        part = acc.astype(jnp.bfloat16).astype(jnp.float32)
        rows.append(part)
        acc = acc - part
    rows.append(jnp.zeros_like(acc))
    count, start = keys.shape[1], ref.shape[0] - TAIL
    ref[start:, :count] = jnp.concatenate(rows, axis=0).astype(jnp.bfloat16)
    ref[start:, count:] = jnp.zeros((TAIL, ref.shape[1] - count), jnp.bfloat16)


def best_of(best, row_key, low, rows, others, key_col):
    scores = lax.dot_general(
        others, rows, (((1,), (1,)), ((), ())), preferred_element_type=jnp.float32
    )
    count = rows.shape[0]
    key = jnp.concatenate([key_col] * (-(-count // 128)), axis=1)[:, :count]
    allowed = (key < row_key) & (key >= low)
    masked = jnp.where(allowed, scores, jnp.float32(-1.0))
    return jnp.maximum(best, jnp.max(masked, axis=0, keepdims=True))


def lay_kernel(count, starts, keyed, *refs):
    first = 0
    if keyed:
        refs[-1][...] = key_columns(refs[count][...])
        refs = refs[:count] + refs[count + 1 : -1]
    for ref in refs[:count]:
        end = first + ref.shape[0]
        for start, out in zip(starts, refs[count:]):
            low, high = max(first, start), min(end, start + out.shape[0])
            if low < high:
                out[low - start : high - start, :] = ref[low - first : high - first, :]
        first = end


def lay(pieces, cuts, keys=()):
    width = pieces[0].shape[1]
    total = sum(end - start for start, end in cuts)
    return pl.pallas_call(
        functools.partial(lay_kernel, len(pieces), [start for start, _ in cuts], bool(keys)),
        out_shape=[jax.ShapeDtypeStruct((end - start, width), jnp.bfloat16) for start, end in cuts]
        + [jax.ShapeDtypeStruct((k.shape[1], 128), jnp.int32) for k in keys],
        in_specs=[VMEM] * (len(pieces) + len(keys)),
        out_specs=[VMEM] * (len(cuts) + len(keys)),
        compiler_params=PARAMS,
        cost_estimate=pl.CostEstimate(
            flops=total, bytes_accessed=4 * total * width, transcendentals=0
        ),
        name="lay",
    )(*pieces, *keys)


def visit_kernel(begins, pieces, own_ref, own_columns_ref, *refs):
    piece_refs, out_ref = refs[:pieces], refs[-1]
    count = out_ref.shape[0] - TAIL
    last = piece_refs[-1][:count, :]
    rows = jnp.concatenate([*[r[...] for r in piece_refs[:-1]], last], axis=0)
    acc = jnp.full((1, rows.shape[0]), -1.0, jnp.float32)
    if begins:
        keys = refs[pieces][...]
    else:
        keys, acc = read_tail(piece_refs[-1], rows.shape[0])
        refs[pieces][...] = keys
    low = keys & jnp.int32(-label_stride)
    acc = best_of(acc, keys, low, rows, own_ref[...], own_columns_ref[...])
    out_ref[:count, :] = last
    write_tail(out_ref, keys, acc)


def visit(own, pieces, keys=None):
    begins = keys is not None
    total, width = own[0].shape
    rows = pieces[-1].shape[0] + (TAIL if begins else 0)
    operands = [*own, *pieces] + ([keys] if begins else [])
    out_shape = [] if begins else [jax.ShapeDtypeStruct((1, total), jnp.int32)]
    out_shape.append(jax.ShapeDtypeStruct((rows, width), jnp.bfloat16))
    return pl.pallas_call(
        functools.partial(visit_kernel, begins, len(pieces)),
        out_shape=out_shape,
        in_specs=[VMEM] * len(operands),
        out_specs=[VMEM] * len(out_shape),
        compiler_params=PARAMS,
        cost_estimate=pl.CostEstimate(
            flops=total, bytes_accessed=4 * total * width, transcendentals=0
        ),
        name="visit",
    )(*operands)


def columns_kernel(keys_ref, columns_ref):
    columns_ref[...] = key_columns(keys_ref[...])


def columns_of(keys):
    return pl.pallas_call(
        columns_kernel,
        out_shape=jax.ShapeDtypeStruct((keys.shape[1], 128), jnp.int32),
        in_specs=[VMEM],
        out_specs=VMEM,
        compiler_params=PARAMS,
        name="columns",
    )(keys)


def meet_kernel(first_row, pieces, keys_ref, *refs):
    out_ref = refs[-1]
    count = out_ref.shape[1]
    rows = jnp.concatenate([r[...] for r in refs[:pieces]], axis=0)[:count]
    row_key = keys_ref[:, first_row : first_row + count]
    low = row_key & jnp.int32(-label_stride)
    best = jnp.full((1, count), -1.0, jnp.float32)
    for at in range(pieces, len(refs) - 1, 2):
        best = best_of(best, row_key, low, rows, refs[at][...], refs[at + 1][...])
    out_ref[...] = best


def meet(keys, first_row, count, pieces, blocks):
    width = pieces[0].shape[1]
    operands = [keys, *pieces]
    for whole, columns in blocks:
        operands += [whole, columns]
    others = sum(whole.shape[0] for whole, _ in blocks)
    return pl.pallas_call(
        functools.partial(meet_kernel, first_row, len(pieces)),
        out_shape=jax.ShapeDtypeStruct((1, count), jnp.float32),
        in_specs=[VMEM] * len(operands),
        out_specs=VMEM,
        compiler_params=PARAMS,
        cost_estimate=pl.CostEstimate(
            flops=2 * count * others * width,
            bytes_accessed=2 * (count + others) * width,
            transcendentals=0,
        ),
        name="meet",
    )(*operands)


def join_kernel(pieces, keys_ref, facing_keys_ref, facing_ref, front_ref, back_ref, *refs):
    out_ref = refs[-1]
    keys = keys_ref[...]
    rows = jnp.concatenate([r[...] for r in refs[:pieces]], axis=0)[: keys.shape[1]]
    low = keys & jnp.int32(-label_stride)
    columns = key_columns(facing_keys_ref[...])[: facing_ref.shape[0]]
    best = jnp.concatenate([front_ref[...], back_ref[...]], axis=1)
    best = jnp.maximum(best, read_tail(refs[pieces - 1], best.shape[1])[1])
    best = best_of(best, keys, low, rows, facing_ref[...], columns)
    out_ref[...] = jnp.broadcast_to(best[:, None, :], out_ref.shape)


def join(keys, facing_keys, facing, front, back, pieces, chips):
    total = keys.shape[1]
    operands = [keys, facing_keys, facing, front, back, *pieces]
    return pl.pallas_call(
        functools.partial(join_kernel, len(pieces)),
        out_shape=jax.ShapeDtypeStruct((chips, 1, total), jnp.float32),
        in_specs=[VMEM] * len(operands),
        out_specs=VMEM,
        compiler_params=PARAMS,
        name="join",
    )(*operands)


def limit_kernel(root, index_ref, limit_ref):
    limit = jnp.zeros(limit_ref.shape, jnp.float32)
    for entry in range(LIMITS):
        value = jnp.float32((2.0 + 0.5 * entry) / root)
        limit = jnp.where(index_ref[0] == entry, value, limit)
    limit_ref[...] = limit


def limit_of(limit_index, root):
    return pl.pallas_call(
        functools.partial(limit_kernel, root),
        out_shape=jax.ShapeDtypeStruct((1, 128), jnp.float32),
        in_specs=[pl.BlockSpec(memory_space=pltpu.SMEM)],
        out_specs=VMEM,
        compiler_params=PARAMS,
        name="limit",
    )(limit_index)


def finish_kernel(width, limit_ref, mine_ref, theirs_ref, best_ref, share_ref):
    blocks, rows = mine_ref.shape
    half = rows // 2
    core, blk = lax.axis_index("sub"), lax.axis_index("blk")
    limit = limit_ref[:, :1]
    quarter = blocks // 4

    def turned(x, by):
        return jnp.concatenate([x[by:], x[:by]], axis=0)

    mine, theirs = mine_ref[...], theirs_ref[...]
    mine = jnp.concatenate([mine[:, half:], mine[:, :half]], axis=1)
    up, down = quarter, blocks - quarter
    best = jnp.where(
        core == 0,
        jnp.maximum(turned(mine, down), turned(theirs, up)),
        jnp.maximum(turned(mine, up), turned(theirs, down)),
    )
    kept = jax.nn.sigmoid(2.0 * width * (limit - best))
    total = jnp.sum(jnp.sum(kept, axis=0, keepdims=True), axis=1, keepdims=True)
    share_ref[...] = total / (blocks * rows)
    at = lax.broadcasted_iota(jnp.int32, best.shape, 0)
    own = jnp.max(jnp.where(at == blk, best, jnp.float32(-2.0)), axis=0, keepdims=True)
    best_ref[...] = own[:, :half]


def finish(limit, mine, theirs, width):
    rows = mine.shape[1]
    return pl.pallas_call(
        functools.partial(finish_kernel, width),
        out_shape=[
            jax.ShapeDtypeStruct((1, rows // 2), jnp.float32),
            jax.ShapeDtypeStruct((1, 1), jnp.float32),
        ],
        in_specs=[VMEM] * 3,
        out_specs=[VMEM, VMEM],
        compiler_params=PARAMS,
        name="finish",
    )(limit, mine, theirs)


def program(embeddings, member_key, limit_index):
    chips, cores = lax.axis_size("blk"), lax.axis_size("sub")
    rows, width = embeddings.shape
    hops = chips // 4

    def moves(by, change):
        pairs = []
        for c in range(chips):
            for core, to in ((0, (c + by) % chips), (1, (c - by) % chips)):
                pairs.append((cores * c + core, cores * to + (1 - core if change else core)))
        return pairs

    def send(x, by, change=False):
        return lax.ppermute(x, ("blk", "sub"), moves(by, change))

    def across(x):
        return lax.ppermute(x, "sub", [(0, 1), (1, 0)])

    total = cores * rows
    size = total // PIECES
    cuts = [(n * size, (n + 1) * size) for n in range(PIECES)]
    keys = member_key.reshape(1, rows)
    keys = jnp.concatenate([keys, across(keys)], axis=1)
    mine = normalize(embeddings, (size, rows - size))
    theirs = [across(m) for m in mine]
    (second,) = lay([mine[1], theirs[0]], [(0, size)])
    *rest, whole = lay([*mine, *theirs], [*cuts[2:], (0, total)])
    block = [mine[0], second, *rest]
    own = (whole, columns_of(keys))
    held = [own]
    (block[-1],) = visit(own, block, keys)
    for _ in range(1, hops):
        block = [send(b, 1) for b in block]
        keys, last = visit(own, block)
        held.append(lay(block, [(0, total)], [keys]))
        block[-1] = last
    last_keys = send(keys, 1, True)
    next_keys = send(keys, 1)
    block = [send(b, 1, True) for b in block]
    (first,) = lay(block[:-1], [(0, rows)])
    split = size * (PIECES - 1)
    front = meet(last_keys, 0, split, block[:-1], held)
    first, front = lax.optimization_barrier((first, front))
    facing = across(first)
    back = meet(last_keys, split, size, block[-1:], held)
    everyone = join(last_keys, next_keys, facing, front, back, block, chips)

    limit = limit_of(limit_index, math.sqrt(width))
    gathered = lax.all_to_all(everyone, "blk", 0, 0, tiled=True).reshape(chips, -1)
    other_side = across(gathered)
    root = math.sqrt(width)
    best, share = finish(limit, gathered, other_side, root)
    return (best.reshape(-1), share.reshape(1))


def solution(mesh):
    in_specs = (P(("groups", "blk", "sub"), None), P(("groups", "blk", "sub")), P("groups"))
    out_specs = (P(("groups", "blk", "sub")), P("groups"))
    return jax.shard_map(
        program, mesh=mesh, in_specs=in_specs, out_specs=out_specs, check_vma=False
    )
```
